16 devices in a mesh: dp: 2 (over y, z), tp: 8 (over x, core).
Axes of the slice: x: 4, y: 2, z: 1, core: 2. Of those that a mesh axis runs over, the one named last changes fastest.
The devices are a block of a 4x4x8 slice.
Arguments:
- x: bfloat16 [64, 256, 1024], P('dp', 'tp'), parts along dimension 0
- d_out: bfloat16 [64, 256, 1024], P('dp', 'tp'), parts along dimension 0
- ln1_gain: float32 [1024], replicated
- ln1_bias: float32 [1024], replicated
- w_q: bfloat16 [1024, 16, 64], P(None, 'tp')
- b_q: bfloat16 [16, 64], P('tp')
- w_k: bfloat16 [1024, 16, 64], P(None, 'tp')
- w_v: bfloat16 [1024, 16, 64], P(None, 'tp')
- b_v: bfloat16 [16, 64], P('tp')
- w_o: bfloat16 [16, 64, 1024], P('tp')
- b_o: bfloat16 [1024], replicated
- ln2_gain: float32 [1024], replicated
- ln2_bias: float32 [1024], replicated
- w_1: bfloat16 [1024, 4096], P(None, 'tp')
- b_1: bfloat16 [4096], P('tp')
- w_2: bfloat16 [4096, 1024], P('tp')
- b_2: bfloat16 [1024], replicated
Outputs:
- output 1: bfloat16 [64, 256, 1024], P('dp', 'tp'), parts along dimension 0
- output 2: bfloat16 [64, 256, 1024], P('dp', 'tp'), parts along dimension 0
- output 3: float32 [2048], P('dp'), parts along dimension 0
- output 4: float32 [2048], P('dp'), parts along dimension 0
- output 5: bfloat16 [2048, 16, 64], P('dp', 'tp'), parts along dimension 0
- output 6: bfloat16 [32, 64], P(('dp', 'tp')), parts along dimension 0
- output 7: bfloat16 [2048, 16, 64], P('dp', 'tp'), parts along dimension 0
- output 8: bfloat16 [2048, 16, 64], P('dp', 'tp'), parts along dimension 0
- output 9: bfloat16 [32, 64], P(('dp', 'tp')), parts along dimension 0
- output 10: bfloat16 [32, 64, 1024], P(('dp', 'tp')), parts along dimension 0
- output 11: bfloat16 [2048], P('dp'), parts along dimension 0
- output 12: float32 [2048], P('dp'), parts along dimension 0
- output 13: float32 [2048], P('dp'), parts along dimension 0
- output 14: bfloat16 [2048, 4096], P('dp', 'tp'), parts along dimension 0
- output 15: bfloat16 [8192], P(('dp', 'tp')), parts along dimension 0
- output 16: bfloat16 [8192, 1024], P(('dp', 'tp')), parts along dimension 0
- output 17: bfloat16 [2048], P('dp'), parts along dimension 0
There are 2 independent parts. The reference program is written for one: setup_inputs(seed, part) draws one part's arguments, and reference() takes and returns one part's arrays. A program takes and returns all parts, laid end to end along the dimension named above; an argument that names none is the same for every part.
All inputs are finite; a program needn't handle non-finite values.
Results may differ from the reference program's by a relative error of at most 0.0185995.
Values are sent between devices in bfloat16 or wider.
A program may use at most 768 MiB of HBM per device.

```python
import math
import jax
import jax.numpy as jnp
from jax import lax

IMAGES = 32
PATCHES = 256
WIDTH = 1024
NUM_HEADS = 16
HEAD_DIM = 64
MLP_DIM = 4096
LN_EPS = 1e-6
ATT_SCALE = 1.0 / math.sqrt(HEAD_DIM)
TOKENS = IMAGES * PATCHES


def draw_normal(key, shape, scale):
    return jax.random.normal(key, shape, jnp.float32) * scale


def setup_inputs(seed: int = 0, part: int = 0) -> dict:
    part_key = jax.random.fold_in(jax.random.key(seed), part)
    act_keys = jax.random.split(part_key, 4)
    wt_keys = jax.random.split(jax.random.key(seed + 1), 15)
    act_shape = (IMAGES, PATCHES, WIDTH)
    row_scale = jnp.exp(draw_normal(act_keys[0], (IMAGES, PATCHES, 1), 0.5))
    row_shift = draw_normal(act_keys[1], (IMAGES, PATCHES, 1), 0.5)
    x = (draw_normal(act_keys[2], act_shape, 1.0) * row_scale + row_shift).astype(jnp.bfloat16)
    d_out = draw_normal(act_keys[3], act_shape, 1.0).astype(jnp.bfloat16)
    in_scale = WIDTH ** -0.5
    qk_scale = in_scale * math.sqrt(math.sqrt(math.log(PATCHES / 8.0)))
    head_w = (WIDTH, NUM_HEADS, HEAD_DIM)
    head_b = (NUM_HEADS, HEAD_DIM)
    return {
        'x': x,
        'd_out': d_out,
        'ln1_gain': 1.0 + draw_normal(wt_keys[0], (WIDTH,), 0.25),
        'ln1_bias': draw_normal(wt_keys[1], (WIDTH,), 0.3),
        'w_q': draw_normal(wt_keys[2], head_w, qk_scale).astype(jnp.bfloat16),
        'b_q': draw_normal(wt_keys[3], head_b, 0.5).astype(jnp.bfloat16),
        'w_k': draw_normal(wt_keys[4], head_w, qk_scale).astype(jnp.bfloat16),
        'w_v': draw_normal(wt_keys[5], head_w, in_scale).astype(jnp.bfloat16),
        'b_v': draw_normal(wt_keys[6], head_b, 0.5).astype(jnp.bfloat16),
        'w_o': draw_normal(wt_keys[7], (NUM_HEADS, HEAD_DIM, WIDTH), 2.5 * in_scale).astype(jnp.bfloat16),
        'b_o': draw_normal(wt_keys[8], (WIDTH,), 0.5).astype(jnp.bfloat16),
        'ln2_gain': 1.0 + draw_normal(wt_keys[9], (WIDTH,), 0.25),
        'ln2_bias': draw_normal(wt_keys[10], (WIDTH,), 0.3),
        'w_1': draw_normal(wt_keys[11], (WIDTH, MLP_DIM), in_scale).astype(jnp.bfloat16),
        'b_1': draw_normal(wt_keys[12], (MLP_DIM,), 0.5).astype(jnp.bfloat16),
        'w_2': draw_normal(wt_keys[13], (MLP_DIM, WIDTH), 1.5 * MLP_DIM ** -0.5).astype(jnp.bfloat16),
        'b_2': draw_normal(wt_keys[14], (WIDTH,), 0.5).astype(jnp.bfloat16),
    }


def layer_norm(rows, ln_gain, ln_bias):
    row_mean = jnp.mean(rows, axis=-1, keepdims=True)
    centered = rows - row_mean
    variance = jnp.mean(centered * centered, axis=-1, keepdims=True)
    return centered * lax.rsqrt(variance + LN_EPS) * ln_gain + ln_bias


def attend_image(qkv_image):
    queries, keys, values = qkv_image
    scores = jnp.einsum('qhd,khd->hqk', queries.astype(jnp.float32), keys.astype(jnp.float32)) * ATT_SCALE
    probs = jax.nn.softmax(scores, axis=-1).astype(jnp.bfloat16)
    mixed = jnp.einsum('hqk,khd->qhd', probs.astype(jnp.float32), values.astype(jnp.float32))
    return mixed.astype(jnp.bfloat16)


def forward(x, ln1_gain, ln1_bias, w_q, b_q, w_k, w_v, b_v, w_o, b_o, ln2_gain, ln2_bias, w_1, b_1, w_2, b_2):
    x_f32 = x.reshape(TOKENS, WIDTH).astype(jnp.float32)
    h_one = layer_norm(x_f32, ln1_gain, ln1_bias).astype(jnp.bfloat16)
    w_qkv = jnp.concatenate([w_q.reshape(WIDTH, WIDTH), w_k.reshape(WIDTH, WIDTH), w_v.reshape(WIDTH, WIDTH)], axis=1)
    b_qkv = jnp.concatenate([b_q.reshape(WIDTH).astype(jnp.float32), jnp.zeros((WIDTH,), jnp.float32), b_v.reshape(WIDTH).astype(jnp.float32)])
    qkv = (jnp.dot(h_one, w_qkv, preferred_element_type=jnp.float32) + b_qkv).astype(jnp.bfloat16)
    head_shape = (IMAGES, PATCHES, NUM_HEADS, HEAD_DIM)
    queries = qkv[:, :WIDTH].reshape(head_shape)
    keys = qkv[:, WIDTH:2 * WIDTH].reshape(head_shape)
    values = qkv[:, 2 * WIDTH:].reshape(head_shape)
    mixed = lax.map(attend_image, (queries, keys, values)).reshape(TOKENS, WIDTH)
    attn_out = jnp.dot(mixed, w_o.reshape(WIDTH, WIDTH), preferred_element_type=jnp.float32)
    x_mid = (x_f32 + attn_out + b_o).astype(jnp.bfloat16)
    mid_f32 = x_mid.astype(jnp.float32)
    h_two = layer_norm(mid_f32, ln2_gain, ln2_bias).astype(jnp.bfloat16)
    pre_act = (jnp.dot(h_two, w_1, preferred_element_type=jnp.float32) + b_1).astype(jnp.bfloat16)
    hidden = jax.nn.gelu(pre_act.astype(jnp.float32), approximate=True).astype(jnp.bfloat16)
    mlp_out = jnp.dot(hidden, w_2, preferred_element_type=jnp.float32)
    y_out = (mid_f32 + mlp_out + b_2).astype(jnp.bfloat16)
    return y_out.reshape(IMAGES, PATCHES, WIDTH)


def reference(x, d_out, ln1_gain, ln1_bias, w_q, b_q, w_k, w_v, b_v, w_o, b_o, ln2_gain, ln2_bias, w_1, b_1, w_2, b_2):
    y_out, pullback = jax.vjp(forward, x, ln1_gain, ln1_bias, w_q, b_q, w_k, w_v, b_v, w_o, b_o, ln2_gain, ln2_bias, w_1, b_1, w_2, b_2)
    (grad_x, grad_ln1_gain, grad_ln1_bias, grad_w_q, grad_b_q, grad_w_k, grad_w_v, grad_b_v, grad_w_o, grad_b_o,
     grad_ln2_gain, grad_ln2_bias, grad_w_1, grad_b_1, grad_w_2, grad_b_2) = pullback(d_out)
    return (y_out, grad_x, grad_ln1_gain, grad_ln1_bias, grad_w_q, grad_b_q, grad_w_k, grad_w_v, grad_b_v, grad_w_o, grad_b_o,
            grad_ln2_gain, grad_ln2_bias, grad_w_1, grad_b_1, grad_w_2, grad_b_2)
```

```python
import math
import jax
import jax.numpy as jnp
from jax import lax
from jax.sharding import PartitionSpec as P

LN_EPS = 1e-6
F32 = jnp.float32
BF16 = jnp.bfloat16


def layer_norm(rows, ln_gain, ln_bias):
    row_mean = jnp.mean(rows, axis=-1, keepdims=True)
    centered = rows - row_mean
    variance = jnp.mean(centered * centered, axis=-1, keepdims=True)
    return centered * lax.rsqrt(variance + LN_EPS) * ln_gain + ln_bias


def gelu_tanh(pre_act):
    return jax.nn.gelu(pre_act, approximate=True)


def attention_core(queries, keys, values):
    att_scale = 1.0 / math.sqrt(queries.shape[-1])
    scores = jnp.einsum('bqhd,bkhd->bhqk', queries, keys, preferred_element_type=F32) * att_scale
    probs = jax.nn.softmax(scores, axis=-1).astype(BF16)
    mixed = jnp.einsum('bhqk,bkhd->bqhd', probs, values, preferred_element_type=F32)
    return mixed.astype(BF16)


def dot(a, b, ca, cb):
    return lax.dot_general(a, b, (((ca,), (cb,)), ((), ())), preferred_element_type=F32)


def solution(mesh):
    act_spec = P('dp', 'tp', None)
    replicated = P()
    head_w = P(None, 'tp', None)
    head_b = P('tp', None)
    grad_head_w = P('dp', 'tp', None)
    grad_head_b = P(('dp', 'tp'), None)
    grad_vec = P('dp')
    in_specs = (act_spec, act_spec, replicated, replicated, head_w, head_b, head_w, head_w, head_b,
                P('tp', None, None), replicated, replicated, replicated, P(None, 'tp'), P('tp'), P('tp', None), replicated)
    out_specs = (act_spec, act_spec, grad_vec, grad_vec, grad_head_w, grad_head_b, grad_head_w, grad_head_w, grad_head_b,
                 P(('dp', 'tp'), None, None), grad_vec, grad_vec, grad_vec, P('dp', 'tp'), P(('dp', 'tp')),
                 P(('dp', 'tp'), None), grad_vec)
    tp = mesh.shape['tp']

    def gather_rows(rows):
        return lax.all_gather(rows, 'tp', axis=0, tiled=True)

    def scatter_rows(rows):
        return lax.psum_scatter(rows, 'tp', scatter_dimension=0, tiled=True)

    def layer_step(x, d_out, ln1_gain, ln1_bias, w_q, b_q, w_k, w_v, b_v, w_o, b_o, ln2_gain, ln2_bias, w_1, b_1, w_2, b_2):
        width, my_heads, head_dim = w_q.shape
        cols = my_heads * head_dim
        hid = w_1.shape[1]
        images, patches = x.shape[0] // tp, x.shape[1] * tp
        tokens = images * patches

        def to_images(t):
            return lax.all_to_all(t, 'tp', 0, 1, tiled=True).reshape(tokens, width)

        def to_tokens(t):
            return lax.all_to_all(t.reshape(images, patches, width), 'tp', 1, 0, tiled=True)

        x_img = to_images(x)
        qkv_rows = jnp.concatenate([w_q.reshape(width, cols).T, w_k.reshape(width, cols).T, w_v.reshape(width, cols).T], axis=0)
        w_qkv = gather_rows(qkv_rows)
        b_small = jnp.concatenate([b_q.reshape(cols), jnp.zeros((cols,), BF16), b_v.reshape(cols), b_1])
        b_all = lax.all_gather(b_small, 'tp')
        b_qkv = b_all[:, :3 * cols].reshape(tp * 3 * cols)
        b_1_all = b_all[:, 3 * cols:].reshape(tp * hid)
        wo_all = gather_rows(w_o.reshape(cols, width))
        w1_all = gather_rows(w_1.T)
        w2_all = gather_rows(w_2)
        d_out_img = to_images(d_out)

        x_f32 = x_img.astype(F32)
        h_one_f, ln1_pull = jax.vjp(layer_norm, x_f32, ln1_gain, ln1_bias)
        h_one = h_one_f.astype(BF16)
        qkv = (dot(h_one, w_qkv, 1, 1) + b_qkv.astype(F32)).astype(BF16)
        split = qkv.reshape(images, patches, tp, 3, my_heads, head_dim)

        def pick(i):
            return split[:, :, :, i].reshape(images, patches, tp * my_heads, head_dim)

        mixed, attn_pull = jax.vjp(attention_core, pick(0), pick(1), pick(2))
        mixed = mixed.reshape(tokens, tp * cols)
        x_mid = (x_f32 + dot(mixed, wo_all, 1, 0) + b_o.astype(F32)).astype(BF16)
        mid_f32 = x_mid.astype(F32)
        h_two_f, ln2_pull = jax.vjp(layer_norm, mid_f32, ln2_gain, ln2_bias)
        h_two = h_two_f.astype(BF16)
        pre_act = (dot(h_two, w1_all, 1, 1) + b_1_all.astype(F32)).astype(BF16)
        hidden_f, gelu_pull = jax.vjp(gelu_tanh, pre_act.astype(F32))
        hidden = hidden_f.astype(BF16)
        y_img = (mid_f32 + dot(hidden, w2_all, 1, 0) + b_2.astype(F32)).astype(BF16)
        y_out = to_tokens(y_img)

        grad_w_2 = scatter_rows(dot(hidden, d_out_img, 0, 0)).astype(BF16)
        d_hidden = dot(d_out_img, w2_all, 1, 1).astype(BF16)
        (d_pre_f,) = gelu_pull(d_hidden.astype(F32))
        d_pre = d_pre_f.astype(BF16)
        grad_w_1 = scatter_rows(dot(d_pre, h_two, 0, 0)).astype(BF16).T
        d_h_two = dot(d_pre, w1_all, 1, 0).astype(BF16)
        d_mid_ln, g_ln2_gain, g_ln2_bias = ln2_pull(d_h_two.astype(F32))
        d_mid = (d_out_img.astype(F32) + d_mid_ln).astype(BF16)
        d_mixed = dot(d_mid, wo_all, 1, 1).astype(BF16)
        grad_w_o = scatter_rows(dot(mixed, d_mid, 0, 0)).astype(BF16).reshape(my_heads, head_dim, width)
        d_q, d_k, d_v = attn_pull(d_mixed.reshape(images, patches, tp * my_heads, head_dim))
        d_split = jnp.stack([t.reshape(images, patches, tp, my_heads, head_dim) for t in (d_q, d_k, d_v)], axis=3)
        d_qkv = d_split.reshape(tokens, tp * 3 * cols)
        g_qkv = scatter_rows(dot(d_qkv, h_one, 0, 0)).astype(BF16).reshape(3, cols, width)
        grad_w_q, grad_w_k, grad_w_v = (g_qkv[i].T.reshape(width, my_heads, head_dim) for i in range(3))
        d_h_one = dot(d_qkv, w_qkv, 1, 0).astype(BF16)
        d_in_ln, g_ln1_gain, g_ln1_bias = ln1_pull(d_h_one.astype(F32))
        grad_x = to_tokens((d_mid.astype(F32) + d_in_ln).astype(BF16))

        def token_sum(t):
            return jnp.sum(t, axis=0, dtype=F32)

        vecs = jnp.concatenate([g_ln1_gain, g_ln1_bias, token_sum(d_mid), g_ln2_gain, g_ln2_bias, token_sum(d_out_img),
                                token_sum(d_qkv), token_sum(d_pre)])
        sums = lax.psum(vecs.reshape(-1, width), 'tp').reshape(-1)
        six = [sums[i * width:(i + 1) * width] for i in range(6)]
        me = lax.axis_index('tp')
        g_b_qkv = lax.dynamic_slice(sums, (6 * width + me * 3 * cols,), (3 * cols,)).astype(BF16)
        grad_b_q = g_b_qkv[:cols].reshape(my_heads, head_dim)
        grad_b_v = g_b_qkv[2 * cols:].reshape(my_heads, head_dim)
        grad_b_1 = lax.dynamic_slice(sums, (6 * width + tp * 3 * cols + me * hid,), (hid,)).astype(BF16)
        return (y_out, grad_x, six[0], six[1], grad_w_q, grad_b_q, grad_w_k, grad_w_v, grad_b_v, grad_w_o,
                six[2].astype(BF16), six[3], six[4], grad_w_1, grad_b_1, grad_w_2, six[5].astype(BF16))

    return jax.shard_map(layer_step, mesh=mesh, in_specs=in_specs, out_specs=out_specs, check_vma=False)
```

```python
import functools
import math
import jax
import jax.numpy as jnp
from jax import lax
from jax.experimental import pallas as pl
from jax.sharding import PartitionSpec as P

LN_EPS = 1e-6
F32 = jnp.float32
BF16 = jnp.bfloat16
PAD = 16


def layer_norm(rows, ln_gain, ln_bias):
    row_mean = jnp.mean(rows, axis=-1, keepdims=True)
    centered = rows - row_mean
    variance = jnp.mean(centered * centered, axis=-1, keepdims=True)
    return centered * lax.rsqrt(variance + LN_EPS) * ln_gain + ln_bias


def gelu_tanh(pre_act):
    return jax.nn.gelu(pre_act, approximate=True)


def after(values, token):
    return lax.optimization_barrier((*values, token))[:len(values)]


def dot(a, b, ca, cb):
    return lax.dot_general(a, b, (((ca,), (cb,)), ((), ())), preferred_element_type=F32)


def head_lanes(shape, head, head_dim):
    lane = lax.broadcasted_iota(jnp.int32, shape, 1)
    return (lane >= head * head_dim) & (lane < (head + 1) * head_dim)


def attend_kernel(heads, head_dim, qkv_ref, out_ref):
    cols = heads * head_dim
    q, k, v = (qkv_ref[:, i * cols:(i + 1) * cols] for i in range(3))
    scale = 1.0 / math.sqrt(head_dim)
    total = None
    for head in range(heads):
        mine = head_lanes(q.shape, head, head_dim)
        s = dot(jnp.where(mine, q, jnp.zeros_like(q)), k, 1, 1) * scale
        e = jnp.exp(s - jnp.max(s, axis=1, keepdims=True))
        p = (e / jnp.sum(e, axis=1, keepdims=True)).astype(BF16)
        a = dot(p, v, 1, 0)
        total = a if total is None else jnp.where(mine, a, total)
    out_ref[...] = total.astype(BF16)


def attend_back_kernel(heads, head_dim, qkv_ref, da_ref, dqkv_ref):
    cols = heads * head_dim
    q, k, v = (qkv_ref[:, i * cols:(i + 1) * cols] for i in range(3))
    da = da_ref[...]
    scale = 1.0 / math.sqrt(head_dim)
    dq = dk = dv = None
    for head in range(heads):
        mine = head_lanes(q.shape, head, head_dim)
        zero = jnp.zeros_like(q)
        s = dot(jnp.where(mine, k, zero), q, 1, 1) * scale
        e = jnp.exp(s - jnp.max(s, axis=0, keepdims=True))
        p32 = e / jnp.sum(e, axis=0, keepdims=True)
        dv_h = dot(p32.astype(BF16), da, 1, 0)
        dp = dot(jnp.where(mine, v, zero), da, 1, 1).astype(BF16).astype(F32)
        ds = p32 * (dp - jnp.sum(dp * p32, axis=0, keepdims=True))
        ds = (ds * scale).astype(BF16)
        dk_h = dot(ds, q, 1, 0)
        dq_h = dot(ds, k, 0, 0)
        if head == 0:
            dq, dk, dv = dq_h, dk_h, dv_h
        else:
            dq, dk, dv = jnp.where(mine, dq_h, dq), jnp.where(mine, dk_h, dk), jnp.where(mine, dv_h, dv)
    for i, d in enumerate((dq, dk, dv)):
        dqkv_ref[:, i * cols:(i + 1) * cols] = d.astype(BF16)


def attend(qkv, images, heads, head_dim):
    tokens, wide = qkv.shape
    patches, cols = tokens // images, heads * head_dim
    blocks = wide // (3 * cols)
    return pl.pallas_call(
        functools.partial(attend_kernel, heads, head_dim),
        grid=(images, blocks),
        in_specs=[pl.BlockSpec((patches, 3 * cols), lambda i, j: (i, j))],
        out_specs=pl.BlockSpec((patches, cols), lambda i, j: (i, j)),
        out_shape=jax.ShapeDtypeStruct((tokens, blocks * cols), BF16),
        cost_estimate=pl.CostEstimate(flops=images * blocks * heads * patches * patches * 1024, bytes_accessed=8 * tokens * blocks * cols,
                                      transcendentals=0),
        name="attend",
    )(qkv)


def attend_back(qkv, d_mixed, images, heads, head_dim):
    tokens, wide = qkv.shape
    patches, cols = tokens // images, heads * head_dim
    blocks = wide // (3 * cols)
    return pl.pallas_call(
        functools.partial(attend_back_kernel, heads, head_dim),
        grid=(images, blocks),
        in_specs=[pl.BlockSpec((patches, 3 * cols), lambda i, j: (i, j)), pl.BlockSpec((patches, cols), lambda i, j: (i, j))],
        out_specs=pl.BlockSpec((patches, 3 * cols), lambda i, j: (i, j)),
        out_shape=jax.ShapeDtypeStruct((tokens, wide), BF16),
        cost_estimate=pl.CostEstimate(flops=images * blocks * heads * patches * patches * 2048, bytes_accessed=14 * tokens * blocks * cols,
                                      transcendentals=0),
        name="attend_back",
    )(qkv, d_mixed)


def solution(mesh):
    act_spec = P('dp', 'tp', None)
    replicated = P()
    head_w = P(None, 'tp', None)
    head_b = P('tp', None)
    grad_head_w = P('dp', 'tp', None)
    grad_head_b = P(('dp', 'tp'), None)
    grad_vec = P('dp')
    in_specs = (act_spec, act_spec, replicated, replicated, head_w, head_b, head_w, head_w, head_b,
                P('tp', None, None), replicated, replicated, replicated, P(None, 'tp'), P('tp'), P('tp', None), replicated)
    out_specs = (act_spec, act_spec, grad_vec, grad_vec, grad_head_w, grad_head_b, grad_head_w, grad_head_w, grad_head_b,
                 P(('dp', 'tp'), None, None), grad_vec, grad_vec, grad_vec, P('dp', 'tp'), P(('dp', 'tp')),
                 P(('dp', 'tp'), None), grad_vec)
    tp = mesh.shape['tp']
    chips = tp // 2
    rings = [[2 * i + core for i in range(chips)] for core in range(2)]
    pairs = [(i, i + 1 - 2 * (i % 2)) for i in range(tp)]

    def gather_rows(rows):
        return lax.all_gather(rows, 'tp', axis=0, tiled=True, axis_index_groups=rings)

    def scatter_rows(rows):
        return lax.psum_scatter(rows, 'tp', scatter_dimension=0, tiled=True, axis_index_groups=rings)

    def swap(t):
        return lax.ppermute(t, 'tp', pairs)

    def layer_body(x, d_out, ln1_gain, ln1_bias, w_q, b_q, w_k, w_v, b_v, w_o, b_o, ln2_gain, ln2_bias, w_1, b_1, w_2, b_2):
        width, my_heads, head_dim = w_q.shape
        cols = my_heads * head_dim
        qkv_cols = 3 * cols
        hid = w_1.shape[1]
        images, patches = x.shape[0] // tp, x.shape[1] * tp
        tokens = images * patches

        def to_images(t):
            return lax.all_to_all(t.reshape(tp, images, patches // tp, width), 'tp', 0, 0, tiled=True)

        def join_tokens(blocks):
            return blocks.swapaxes(0, 1).reshape(tokens, width)

        def to_tokens(t):
            return lax.all_to_all(t.reshape(images, patches, width), 'tp', 1, 0, tiled=True)

        def both(mine, token=None):
            return mine, swap(mine if token is None else after((mine,), token)[0])

        bias_row = jnp.concatenate([b_q.reshape(cols), jnp.zeros((cols,), BF16), b_v.reshape(cols), b_1,
                                    jnp.zeros((width - qkv_cols - hid,), BF16)])
        qkv_rows = jnp.concatenate([w_q.reshape(width, cols).T, w_k.reshape(width, cols).T, w_v.reshape(width, cols).T,
                                    jnp.broadcast_to(bias_row[None], (PAD, width))], axis=0)
        packed = both(gather_rows(qkv_rows))
        x_img = lax.optimization_barrier(join_tokens(to_images(x)))
        wo_mine, w1_mine, w2_mine = gather_rows(w_o.reshape(cols, width)), gather_rows(w_1.T), gather_rows(w_2)

        w_qkv, b_qkv, b_1_all = [], [], []
        for half in packed:
            blocks = half.reshape(chips, qkv_cols + PAD, width)
            w_qkv.append(blocks[:, :qkv_cols].reshape(chips * qkv_cols, width))
            b_qkv.append(blocks[:, qkv_cols, :qkv_cols].reshape(chips * qkv_cols).astype(F32))
            b_1_all.append(blocks[:, qkv_cols, qkv_cols:qkv_cols + hid].reshape(chips * hid).astype(F32))

        x_f32 = x_img.astype(F32)
        h_one_f, ln1_pull = jax.vjp(layer_norm, x_f32, ln1_gain, ln1_bias)
        h_one = h_one_f.astype(BF16)
        qkv = [(dot(h_one, w, 1, 1) + b).astype(BF16) for w, b in zip(w_qkv, b_qkv)]
        d_moved = to_images(after((d_out,), qkv[0])[0])
        wo = both(wo_mine, qkv[0])
        mixed = [attend(t, images, my_heads, head_dim) for t in qkv]
        w1 = both(w1_mine, mixed[1])
        x_mid = (x_f32 + dot(mixed[0], wo[0], 1, 0) + dot(mixed[1], wo[1], 1, 0) + b_o.astype(F32)).astype(BF16)
        mid_f32 = x_mid.astype(F32)
        h_two_f, ln2_pull = jax.vjp(layer_norm, mid_f32, ln2_gain, ln2_bias)
        h_two = h_two_f.astype(BF16)
        pre_act = [(dot(h_two, w, 1, 1) + b).astype(BF16) for w, b in zip(w1, b_1_all)]
        gelus = [jax.vjp(gelu_tanh, t.astype(F32)) for t in pre_act]
        hidden = [g[0].astype(BF16) for g in gelus]

        w2 = both(w2_mine, hidden[1])
        d_out_img = lax.optimization_barrier(join_tokens(after((d_moved,), hidden[0])[0]))
        theirs_2 = dot(hidden[1], d_out_img, 0, 0)
        w2_late = after(w2, theirs_2)
        d_hidden = [dot(d_out_img, w, 1, 1).astype(BF16) for w in w2_late]
        sum_2 = dot(hidden[0], d_out_img, 0, 0) + swap(theirs_2)
        grad_w_2 = scatter_rows(sum_2).astype(BF16)
        d_pre = [g[1](d.astype(F32))[0].astype(BF16) for g, d in zip(gelus, d_hidden)]
        (h_two_late,) = after((h_two,), sum_2)
        theirs_1 = dot(d_pre[1], h_two_late, 0, 0)
        w1_late = after(w1, theirs_1)
        d_h_two = (dot(d_pre[0], w1_late[0], 1, 0) + dot(d_pre[1], w1_late[1], 1, 0)).astype(BF16)
        sum_1 = dot(d_pre[0], h_two_late, 0, 0) + swap(theirs_1)
        grad_w_1 = scatter_rows(sum_1).astype(BF16).T
        w2_late = after(w2, sum_1)
        y_img = (mid_f32 + dot(hidden[0], w2_late[0], 1, 0) + dot(hidden[1], w2_late[1], 1, 0) + b_2.astype(F32)).astype(BF16)
        y_out = to_tokens(y_img)
        d_mid_ln, g_ln2_gain, g_ln2_bias = ln2_pull(d_h_two.astype(F32))
        d_mid = (d_out_img.astype(F32) + d_mid_ln).astype(BF16)
        mixed_late = after(mixed, sum_1)
        theirs_o = dot(mixed_late[1], d_mid, 0, 0)
        d_mixed = [dot(d_mid, w, 1, 1).astype(BF16) for w in wo]
        sum_o = dot(mixed_late[0], d_mid, 0, 0) + swap(theirs_o)
        grad_w_o = scatter_rows(sum_o).astype(BF16).reshape(my_heads, head_dim, width)
        qkv_late = after(qkv, sum_o)
        d_qkv = [attend_back(t, d, images, my_heads, head_dim) for t, d in zip(qkv_late, d_mixed)]
        theirs_qkv = dot(d_qkv[1], h_one, 0, 0)
        w_qkv_late = after(w_qkv, theirs_qkv)
        d_h_one = (dot(d_qkv[0], w_qkv_late[0], 1, 0) + dot(d_qkv[1], w_qkv_late[1], 1, 0)).astype(BF16)
        sum_qkv = dot(d_qkv[0], h_one, 0, 0) + swap(theirs_qkv)
        g_qkv = scatter_rows(sum_qkv).astype(BF16).reshape(3, cols, width)
        grad_w_q, grad_w_k, grad_w_v = (g_qkv[i].T.reshape(width, my_heads, head_dim) for i in range(3))
        d_in_ln, g_ln1_gain, g_ln1_bias = ln1_pull(d_h_one.astype(F32))
        grad_x = to_tokens((d_mid.astype(F32) + d_in_ln).astype(BF16))

        def token_sum(t):
            return jnp.sum(t, axis=0, dtype=F32)

        me = lax.axis_index('tp')
        core, chip = lax.rem(me, 2), me // 2

        def halves(pair):
            sums = [token_sum(t) for t in pair]
            first = jnp.where(core == 0, sums[0], sums[1])
            second = jnp.where(core == 0, sums[1], sums[0])
            return [first, second]

        vecs = jnp.concatenate([g_ln1_gain, g_ln1_bias, token_sum(d_mid), g_ln2_gain, g_ln2_bias, token_sum(d_out_img)]
                               + halves(d_qkv) + halves(d_pre))
        sums = lax.psum(vecs.reshape(-1, width), 'tp').reshape(-1)
        six = [sums[i * width:(i + 1) * width] for i in range(6)]
        base = 6 * width
        g_b_qkv = lax.dynamic_slice(sums, (base + (core * chips + chip) * qkv_cols,), (qkv_cols,)).astype(BF16)
        grad_b_q = g_b_qkv[:cols].reshape(my_heads, head_dim)
        grad_b_v = g_b_qkv[2 * cols:].reshape(my_heads, head_dim)
        base += tp * qkv_cols
        grad_b_1 = lax.dynamic_slice(sums, (base + (core * chips + chip) * hid,), (hid,)).astype(BF16)
        return (y_out, grad_x, six[0], six[1], grad_w_q, grad_b_q, grad_w_k, grad_w_v, grad_b_v, grad_w_o,
                six[2].astype(BF16), six[3], six[4], grad_w_1, grad_b_1, grad_w_2, six[5].astype(BF16))

    return jax.shard_map(layer_body, mesh=mesh, in_specs=in_specs, out_specs=out_specs, check_vma=False)
```

```python
import functools
import math
import jax
import jax.numpy as jnp
from jax import lax
from jax.experimental import pallas as pl
from jax.experimental.pallas import tpu as pltpu
from jax.sharding import PartitionSpec as P

LN_EPS = 1e-6
F32 = jnp.float32
BF16 = jnp.bfloat16
PAD = 16


def layer_norm(rows, ln_gain, ln_bias):
    row_mean = jnp.mean(rows, axis=-1, keepdims=True)
    centered = rows - row_mean
    variance = jnp.mean(centered * centered, axis=-1, keepdims=True)
    return centered * lax.rsqrt(variance + LN_EPS) * ln_gain + ln_bias


def gelu_tanh(pre_act):
    return jax.nn.gelu(pre_act, approximate=True)


def after(values, token):
    return lax.optimization_barrier((*values, token))[:len(values)]


def dot(a, b, ca, cb):
    return lax.dot_general(a, b, (((ca,), (cb,)), ((), ())), preferred_element_type=F32)


def head_lanes(shape, head, head_dim):
    lane = lax.broadcasted_iota(jnp.int32, shape, 1)
    return (lane >= head * head_dim) & (lane < (head + 1) * head_dim)


def attend_kernel(heads, head_dim, qkv_ref, out_ref):
    cols = heads * head_dim
    q, k, v = (qkv_ref[:, i * cols:(i + 1) * cols] for i in range(3))
    scale = 1.0 / math.sqrt(head_dim)
    total = None
    for head in range(heads):
        mine = head_lanes(q.shape, head, head_dim)
        s = dot(jnp.where(mine, q, jnp.zeros_like(q)), k, 1, 1) * scale
        e = jnp.exp(s - jnp.max(s, axis=1, keepdims=True))
        p = (e / jnp.sum(e, axis=1, keepdims=True)).astype(BF16)
        a = dot(p, v, 1, 0)
        total = a if total is None else jnp.where(mine, a, total)
    out_ref[...] = total.astype(BF16)


def attend_back_kernel(heads, head_dim, qkv_ref, da_ref, dqkv_ref):
    cols = heads * head_dim
    q, k, v = (qkv_ref[:, i * cols:(i + 1) * cols] for i in range(3))
    da = da_ref[...]
    scale = 1.0 / math.sqrt(head_dim)
    dq = dk = dv = None
    for head in range(heads):
        mine = head_lanes(q.shape, head, head_dim)
        zero = jnp.zeros_like(q)
        s = dot(jnp.where(mine, k, zero), q, 1, 1) * scale
        e = jnp.exp(s - jnp.max(s, axis=0, keepdims=True))
        p32 = e / jnp.sum(e, axis=0, keepdims=True)
        dv_h = dot(p32.astype(BF16), da, 1, 0)
        dp = dot(jnp.where(mine, v, zero), da, 1, 1).astype(BF16).astype(F32)
        ds = p32 * (dp - jnp.sum(dp * p32, axis=0, keepdims=True))
        ds = (ds * scale).astype(BF16)
        dk_h = dot(ds, q, 1, 0)
        dq_h = dot(ds, k, 0, 0)
        if head == 0:
            dq, dk, dv = dq_h, dk_h, dv_h
        else:
            dq, dk, dv = jnp.where(mine, dq_h, dq), jnp.where(mine, dk_h, dk), jnp.where(mine, dv_h, dv)
    for i, d in enumerate((dq, dk, dv)):
        dqkv_ref[:, i * cols:(i + 1) * cols] = d.astype(BF16)


def attend(qkv, images, heads, head_dim):
    tokens, wide = qkv.shape
    patches, cols = tokens // images, heads * head_dim
    blocks = wide // (3 * cols)
    return pl.pallas_call(
        functools.partial(attend_kernel, heads, head_dim),
        grid=(images, blocks),
        in_specs=[pl.BlockSpec((patches, 3 * cols), lambda i, j: (i, j))],
        out_specs=pl.BlockSpec((patches, cols), lambda i, j: (i, j)),
        out_shape=jax.ShapeDtypeStruct((tokens, blocks * cols), BF16),
        cost_estimate=pl.CostEstimate(flops=images * blocks * heads * patches * patches * 1024, bytes_accessed=8 * tokens * blocks * cols,
                                      transcendentals=0),
        name="attend",
    )(qkv)


def attend_back(qkv, d_mixed, images, heads, head_dim):
    tokens, wide = qkv.shape
    patches, cols = tokens // images, heads * head_dim
    blocks = wide // (3 * cols)
    return pl.pallas_call(
        functools.partial(attend_back_kernel, heads, head_dim),
        grid=(images, blocks),
        in_specs=[pl.BlockSpec((patches, 3 * cols), lambda i, j: (i, j)), pl.BlockSpec((patches, cols), lambda i, j: (i, j))],
        out_specs=pl.BlockSpec((patches, 3 * cols), lambda i, j: (i, j)),
        out_shape=jax.ShapeDtypeStruct((tokens, wide), BF16),
        cost_estimate=pl.CostEstimate(flops=images * blocks * heads * patches * patches * 2048, bytes_accessed=14 * tokens * blocks * cols,
                                      transcendentals=0),
        name="attend_back",
    )(qkv, d_mixed)


def sum_kernel(n, vec_ref, out_ref, slots, send_sems, recv_sems, local_sem):
    me = lax.axis_index('tp')
    barrier = pltpu.get_barrier_semaphore()
    for step in range(1, n):
        pl.semaphore_signal(barrier, inc=1, device_id={'tp': lax.rem(me + step, n)}, device_id_type=pl.DeviceIdType.MESH)
    pl.semaphore_wait(barrier, n - 1)
    own = pltpu.make_async_copy(vec_ref, slots.at[me], local_sem)
    own.start()
    copies = [pltpu.make_async_remote_copy(src_ref=vec_ref, dst_ref=slots.at[me], send_sem=send_sems.at[step - 1],
                                           recv_sem=recv_sems.at[step - 1], device_id={'tp': lax.rem(me + step, n)},
                                           device_id_type=pl.DeviceIdType.MESH) for step in range(1, n)]
    for copy in copies:
        copy.start()
    own.wait()
    for copy in copies:
        copy.wait()
    total = slots[0]
    for i in range(1, n):
        total = total + slots[i]
    out_ref[...] = total


def sum_over_tp(vecs, n):
    return pl.pallas_call(
        functools.partial(sum_kernel, n),
        out_shape=jax.ShapeDtypeStruct(vecs.shape, F32),
        in_specs=[pl.BlockSpec(memory_space=pltpu.VMEM)],
        out_specs=pl.BlockSpec(memory_space=pltpu.VMEM),
        scratch_shapes=[pltpu.VMEM((n, *vecs.shape), F32), pltpu.SemaphoreType.DMA((n - 1,)), pltpu.SemaphoreType.DMA((n - 1,)),
                        pltpu.SemaphoreType.DMA],
        compiler_params=pltpu.CompilerParams(collective_id=0, has_side_effects=True),
        name="sum_over_tp",
    )(vecs)


def solution(mesh):
    act_spec = P('dp', 'tp', None)
    replicated = P()
    head_w = P(None, 'tp', None)
    head_b = P('tp', None)
    grad_head_w = P('dp', 'tp', None)
    grad_head_b = P(('dp', 'tp'), None)
    grad_vec = P('dp')
    in_specs = (act_spec, act_spec, replicated, replicated, head_w, head_b, head_w, head_w, head_b,
                P('tp', None, None), replicated, replicated, replicated, P(None, 'tp'), P('tp'), P('tp', None), replicated)
    out_specs = (act_spec, act_spec, grad_vec, grad_vec, grad_head_w, grad_head_b, grad_head_w, grad_head_w, grad_head_b,
                 P(('dp', 'tp'), None, None), grad_vec, grad_vec, grad_vec, P('dp', 'tp'), P(('dp', 'tp')),
                 P(('dp', 'tp'), None), grad_vec)
    tp = mesh.shape['tp']
    chips = tp // 2
    rings = [[2 * i + core for i in range(chips)] for core in range(2)]
    pairs = [(i, i + 1 - 2 * (i % 2)) for i in range(tp)]

    def gather_rows(rows):
        return lax.all_gather(rows, 'tp', axis=0, tiled=True, axis_index_groups=rings)

    def scatter_rows(rows):
        return lax.psum_scatter(rows, 'tp', scatter_dimension=0, tiled=True, axis_index_groups=rings)

    def swap(t):
        return lax.ppermute(t, 'tp', pairs)

    def layer_body(x, d_out, ln1_gain, ln1_bias, w_q, b_q, w_k, w_v, b_v, w_o, b_o, ln2_gain, ln2_bias, w_1, b_1, w_2, b_2):
        width, my_heads, head_dim = w_q.shape
        cols = my_heads * head_dim
        qkv_cols = 3 * cols
        my_rows = qkv_cols + cols
        hid = w_1.shape[1]
        images, patches = x.shape[0] // tp, x.shape[1] * tp
        tokens = images * patches

        def to_images(t):
            return lax.all_to_all(t.reshape(tp, images, patches // tp, width), 'tp', 0, 0, tiled=True)

        def join_tokens(blocks):
            return blocks.swapaxes(0, 1).reshape(tokens, width)

        def to_tokens(t):
            blocks = t.reshape(images, tp, patches // tp, width).swapaxes(0, 1)
            return lax.all_to_all(blocks, 'tp', 0, 0, tiled=True).reshape(tp * images, patches // tp, width)

        def token_sum(t):
            return jnp.sum(t, axis=0, dtype=F32)

        def both(mine, token=None):
            return mine, swap(mine if token is None else after((mine,), token)[0])

        bias_row = jnp.concatenate([b_q.reshape(cols), jnp.zeros((cols,), BF16), b_v.reshape(cols), b_1,
                                    jnp.zeros((width - qkv_cols - hid,), BF16)])
        qkv_rows = jnp.concatenate([w_q.reshape(width, cols).T, w_k.reshape(width, cols).T, w_v.reshape(width, cols).T,
                                    w_o.reshape(cols, width), jnp.broadcast_to(bias_row[None], (PAD, width))], axis=0)
        packed = both(gather_rows(qkv_rows))
        x_img = lax.optimization_barrier(join_tokens(to_images(x)))
        w1_mine, w2_mine = gather_rows(w_1.T), gather_rows(w_2)

        w_qkv, wo, b_qkv, b_1_all = [], [], [], []
        for half in packed:
            blocks = half.reshape(chips, my_rows + PAD, width)
            w_qkv.append(blocks[:, :qkv_cols].reshape(chips * qkv_cols, width))
            wo.append(blocks[:, qkv_cols:my_rows].reshape(chips * cols, width))
            b_qkv.append(blocks[:, my_rows, :qkv_cols].reshape(chips * qkv_cols).astype(F32))
            b_1_all.append(blocks[:, my_rows, qkv_cols:qkv_cols + hid].reshape(chips * hid).astype(F32))

        x_f32 = x_img.astype(F32)
        h_one_f, ln1_pull = jax.vjp(layer_norm, x_f32, ln1_gain, ln1_bias)
        h_one = h_one_f.astype(BF16)
        qkv = [(dot(h_one, w, 1, 1) + b).astype(BF16) for w, b in zip(w_qkv, b_qkv)]
        d_moved = to_images(after((d_out,), qkv[0])[0])
        mixed = [attend(t, images, my_heads, head_dim) for t in qkv]
        x_mid = (x_f32 + dot(mixed[0], wo[0], 1, 0) + dot(mixed[1], wo[1], 1, 0) + b_o.astype(F32)).astype(BF16)
        w1 = both(w1_mine, x_mid)
        mid_f32 = x_mid.astype(F32)
        h_two_f, ln2_pull = jax.vjp(layer_norm, mid_f32, ln2_gain, ln2_bias)
        h_two = h_two_f.astype(BF16)
        pre_act = [(dot(h_two, w, 1, 1) + b).astype(BF16) for w, b in zip(w1, b_1_all)]
        gelus = [jax.vjp(gelu_tanh, t.astype(F32)) for t in pre_act]
        hidden = [g[0].astype(BF16) for g in gelus]

        d_out_img = lax.optimization_barrier(join_tokens(after((d_moved,), hidden[0])[0]))
        theirs_2 = dot(hidden[1], d_out_img, 0, 0)
        sum_2 = dot(hidden[0], d_out_img, 0, 0) + swap(theirs_2)
        grad_w_2 = scatter_rows(sum_2).astype(BF16)
        w2 = both(w2_mine, sum_2)
        d_first = dot(d_out_img, after(w2[:1], sum_2)[0], 1, 1).astype(BF16)
        d_hidden = [d_first, dot(d_out_img, after(w2[1:], d_first)[0], 1, 1).astype(BF16)]
        d_pre = [g[1](d.astype(F32))[0].astype(BF16) for g, d in zip(gelus, d_hidden)]
        d_pre_sums = [token_sum(t) for t in d_pre]
        (h_two_late,) = after((h_two,), sum_2)
        theirs_1 = dot(d_pre[1], h_two_late, 0, 0)
        w1_late = after(w1, theirs_1)
        d_h_two = (dot(d_pre[0], w1_late[0], 1, 0) + dot(d_pre[1], w1_late[1], 1, 0)).astype(BF16)
        sum_1 = dot(d_pre[0], h_two_late, 0, 0) + swap(theirs_1)
        grad_w_1 = scatter_rows(sum_1).astype(BF16).T
        w2_late = after(w2, sum_1)
        y_img = (mid_f32 + dot(hidden[0], w2_late[0], 1, 0) + dot(hidden[1], w2_late[1], 1, 0) + b_2.astype(F32)).astype(BF16)
        y_out = to_tokens(y_img)
        d_mid_ln, g_ln2_gain, g_ln2_bias = ln2_pull(d_h_two.astype(F32))
        d_mid = (d_out_img.astype(F32) + d_mid_ln).astype(BF16)
        mixed_late = after(mixed, sum_1)
        theirs_o = dot(mixed_late[1], d_mid, 0, 0)
        d_mixed = [dot(d_mid, w, 1, 1).astype(BF16) for w in wo]
        sum_o = dot(mixed_late[0], d_mid, 0, 0) + swap(theirs_o)
        qkv_late = after(qkv, sum_o)
        d_qkv = [attend_back(t, d, images, my_heads, head_dim) for t, d in zip(qkv_late, d_mixed)]
        theirs_qkv = dot(d_qkv[1], h_one, 0, 0)
        w_qkv_late = after(w_qkv, theirs_qkv)
        d_h_one = (dot(d_qkv[0], w_qkv_late[0], 1, 0) + dot(d_qkv[1], w_qkv_late[1], 1, 0)).astype(BF16)
        sum_qkv = dot(d_qkv[0], h_one, 0, 0) + swap(theirs_qkv)
        sum_all = jnp.concatenate([sum_qkv.reshape(chips, qkv_cols, width), sum_o.reshape(chips, cols, width)], axis=1)
        g_all = scatter_rows(sum_all.reshape(chips * my_rows, width)).astype(BF16)
        grad_w_o = g_all[qkv_cols:].reshape(my_heads, head_dim, width)
        g_qkv = g_all[:qkv_cols].reshape(3, cols, width)
        grad_w_q, grad_w_k, grad_w_v = (g_qkv[i].T.reshape(width, my_heads, head_dim) for i in range(3))
        d_in_ln, g_ln1_gain, g_ln1_bias = ln1_pull(d_h_one.astype(F32))
        grad_x = to_tokens((d_mid.astype(F32) + d_in_ln).astype(BF16))

        me = lax.axis_index('tp')
        core, chip = lax.rem(me, 2), me // 2

        def halves(sums):
            first = jnp.where(core == 0, sums[0], sums[1])
            second = jnp.where(core == 0, sums[1], sums[0])
            return [first, second]

        vecs = jnp.concatenate([g_ln1_gain, g_ln1_bias, token_sum(d_mid), g_ln2_gain, g_ln2_bias, token_sum(d_out_img)]
                               + halves([token_sum(t) for t in d_qkv]) + halves(d_pre_sums))
        sums = sum_over_tp(vecs.reshape(-1, width), tp).reshape(-1)
        six = [sums[i * width:(i + 1) * width] for i in range(6)]
        base = 6 * width
        g_b_qkv = lax.dynamic_slice(sums, (base + (core * chips + chip) * qkv_cols,), (qkv_cols,)).astype(BF16)
        grad_b_q = g_b_qkv[:cols].reshape(my_heads, head_dim)
        grad_b_v = g_b_qkv[2 * cols:].reshape(my_heads, head_dim)
        base += tp * qkv_cols
        grad_b_1 = lax.dynamic_slice(sums, (base + (core * chips + chip) * hid,), (hid,)).astype(BF16)
        return (y_out, grad_x, six[0], six[1], grad_w_q, grad_b_q, grad_w_k, grad_w_v, grad_b_v, grad_w_o,
                six[2].astype(BF16), six[3], six[4], grad_w_1, grad_b_1, grad_w_2, six[5].astype(BF16))

    return jax.shard_map(layer_body, mesh=mesh, in_specs=in_specs, out_specs=out_specs, check_vma=False)
```

```python
import functools
import math
import jax
import jax.numpy as jnp
from jax import lax
from jax.experimental import pallas as pl
from jax.experimental.pallas import tpu as pltpu
from jax.sharding import PartitionSpec as P

LN_EPS = 1e-6
F32 = jnp.float32
BF16 = jnp.bfloat16
PAD = 16


def layer_norm(rows, ln_gain, ln_bias):
    row_mean = jnp.mean(rows, axis=-1, keepdims=True)
    centered = rows - row_mean
    variance = jnp.mean(centered * centered, axis=-1, keepdims=True)
    return centered * lax.rsqrt(variance + LN_EPS) * ln_gain + ln_bias


def gelu_tanh(pre_act):
    return jax.nn.gelu(pre_act, approximate=True)


def after(values, token):
    return lax.optimization_barrier((*values, token))[:len(values)]


def dot(a, b, ca, cb):
    return lax.dot_general(a, b, (((ca,), (cb,)), ((), ())), preferred_element_type=F32)


def head_lanes(shape, head, head_dim):
    lane = lax.broadcasted_iota(jnp.int32, shape, 1)
    return (lane >= head * head_dim) & (lane < (head + 1) * head_dim)


def attend_kernel(blocks, heads, head_dim, qkv_ref, out_ref):
    cols = heads * head_dim
    scale = 1.0 / math.sqrt(head_dim)
    for block in range(blocks):
        base = block * 3 * cols
        q, k, v = (qkv_ref[:, base + i * cols:base + (i + 1) * cols] for i in range(3))
        total = None
        for head in range(heads):
            mine = head_lanes(q.shape, head, head_dim)
            s = dot(jnp.where(mine, q, jnp.zeros_like(q)), k, 1, 1) * scale
            e = jnp.exp(s - jnp.max(s, axis=1, keepdims=True))
            p = (e * (1.0 / jnp.sum(e, axis=1, keepdims=True))).astype(BF16)
            a = dot(p, v, 1, 0)
            total = a if total is None else jnp.where(mine, a, total)
        out_ref[:, block * cols:(block + 1) * cols] = total.astype(BF16)


def attend_back_kernel(blocks, heads, head_dim, qkv_ref, da_ref, dqkv_ref):
    cols = heads * head_dim
    scale = 1.0 / math.sqrt(head_dim)
    for block in range(blocks):
        base = block * 3 * cols
        q, k, v = (qkv_ref[:, base + i * cols:base + (i + 1) * cols] for i in range(3))
        da = da_ref[:, block * cols:(block + 1) * cols]
        dq = dk = dv = None
        for head in range(heads):
            mine = head_lanes(q.shape, head, head_dim)
            zero = jnp.zeros_like(q)
            s = dot(jnp.where(mine, k, zero), q, 1, 1) * scale
            e = jnp.exp(s - jnp.max(s, axis=0, keepdims=True))
            p32 = e * (1.0 / jnp.sum(e, axis=0, keepdims=True))
            dv_h = dot(p32.astype(BF16), da, 1, 0)
            dp = dot(jnp.where(mine, v, zero), da, 1, 1).astype(BF16).astype(F32)
            ds = p32 * (dp - jnp.sum(dp * p32, axis=0, keepdims=True))
            ds = (ds * scale).astype(BF16)
            dk_h = dot(ds, q, 1, 0)
            dq_h = dot(ds, k, 0, 0)
            if head == 0:
                dq, dk, dv = dq_h, dk_h, dv_h
            else:
                dq, dk, dv = jnp.where(mine, dq_h, dq), jnp.where(mine, dk_h, dk), jnp.where(mine, dv_h, dv)
        for i, d in enumerate((dq, dk, dv)):
            dqkv_ref[:, base + i * cols:base + (i + 1) * cols] = d.astype(BF16)


GROUP = 4


def attend(qkv, images, heads, head_dim):
    tokens, wide = qkv.shape
    patches, cols = tokens // images, heads * head_dim
    blocks = wide // (3 * cols)
    group = min(GROUP, blocks)
    return pl.pallas_call(
        functools.partial(attend_kernel, group, heads, head_dim),
        grid=(images, blocks // group),
        in_specs=[pl.BlockSpec((patches, group * 3 * cols), lambda i, j: (i, j))],
        out_specs=pl.BlockSpec((patches, group * cols), lambda i, j: (i, j)),
        out_shape=jax.ShapeDtypeStruct((tokens, blocks * cols), BF16),
        cost_estimate=pl.CostEstimate(flops=images * blocks * heads * patches * patches * 1024, bytes_accessed=8 * tokens * blocks * cols,
                                      transcendentals=0),
        name="attend",
    )(qkv)


def attend_back(qkv, d_mixed, images, heads, head_dim):
    tokens, wide = qkv.shape
    patches, cols = tokens // images, heads * head_dim
    blocks = wide // (3 * cols)
    group = min(GROUP, blocks)
    return pl.pallas_call(
        functools.partial(attend_back_kernel, group, heads, head_dim),
        grid=(images, blocks // group),
        in_specs=[pl.BlockSpec((patches, group * 3 * cols), lambda i, j: (i, j)),
                  pl.BlockSpec((patches, group * cols), lambda i, j: (i, j))],
        out_specs=pl.BlockSpec((patches, group * 3 * cols), lambda i, j: (i, j)),
        out_shape=jax.ShapeDtypeStruct((tokens, wide), BF16),
        cost_estimate=pl.CostEstimate(flops=images * blocks * heads * patches * patches * 2048, bytes_accessed=14 * tokens * blocks * cols,
                                      transcendentals=0),
        name="attend_back",
    )(qkv, d_mixed)


def sum_kernel(n, vec_ref, out_ref, slots, send_sems, recv_sems, local_sem):
    me = lax.axis_index('tp')
    barrier = pltpu.get_barrier_semaphore()
    for step in range(1, n):
        pl.semaphore_signal(barrier, inc=1, device_id={'tp': lax.rem(me + step, n)}, device_id_type=pl.DeviceIdType.MESH)
    pl.semaphore_wait(barrier, n - 1)
    own = pltpu.make_async_copy(vec_ref, slots.at[me], local_sem)
    own.start()
    copies = [pltpu.make_async_remote_copy(src_ref=vec_ref, dst_ref=slots.at[me], send_sem=send_sems.at[step - 1],
                                           recv_sem=recv_sems.at[step - 1], device_id={'tp': lax.rem(me + step, n)},
                                           device_id_type=pl.DeviceIdType.MESH) for step in range(1, n)]
    for copy in copies:
        copy.start()
    own.wait()
    for copy in copies:
        copy.wait()
    total = slots[0]
    for i in range(1, n):
        total = total + slots[i]
    out_ref[...] = total


def sum_over_tp(vecs, n):
    return pl.pallas_call(
        functools.partial(sum_kernel, n),
        out_shape=jax.ShapeDtypeStruct(vecs.shape, F32),
        in_specs=[pl.BlockSpec(memory_space=pltpu.VMEM)],
        out_specs=pl.BlockSpec(memory_space=pltpu.VMEM),
        scratch_shapes=[pltpu.VMEM((n, *vecs.shape), F32), pltpu.SemaphoreType.DMA((n - 1,)), pltpu.SemaphoreType.DMA((n - 1,)),
                        pltpu.SemaphoreType.DMA],
        compiler_params=pltpu.CompilerParams(collective_id=0, has_side_effects=True),
        name="sum_over_tp",
    )(vecs)


def solution(mesh):
    act_spec = P('dp', 'tp', None)
    replicated = P()
    head_w = P(None, 'tp', None)
    head_b = P('tp', None)
    grad_head_w = P('dp', 'tp', None)
    grad_head_b = P(('dp', 'tp'), None)
    grad_vec = P('dp')
    in_specs = (act_spec, act_spec, replicated, replicated, head_w, head_b, head_w, head_w, head_b,
                P('tp', None, None), replicated, replicated, replicated, P(None, 'tp'), P('tp'), P('tp', None), replicated)
    out_specs = (act_spec, act_spec, grad_vec, grad_vec, grad_head_w, grad_head_b, grad_head_w, grad_head_w, grad_head_b,
                 P(('dp', 'tp'), None, None), grad_vec, grad_vec, grad_vec, P('dp', 'tp'), P(('dp', 'tp')),
                 P(('dp', 'tp'), None), grad_vec)
    tp = mesh.shape['tp']
    chips = tp // 2
    rings = [[2 * i + core for i in range(chips)] for core in range(2)]
    pairs = [(i, i + 1 - 2 * (i % 2)) for i in range(tp)]

    def gather_rows(rows):
        return lax.all_gather(rows, 'tp', axis=0, tiled=True, axis_index_groups=rings)

    def scatter_rows(rows):
        return lax.psum_scatter(rows, 'tp', scatter_dimension=0, tiled=True, axis_index_groups=rings)

    def swap(t):
        return lax.ppermute(t, 'tp', pairs)

    def layer_body(x, d_out, ln1_gain, ln1_bias, w_q, b_q, w_k, w_v, b_v, w_o, b_o, ln2_gain, ln2_bias, w_1, b_1, w_2, b_2):
        width, my_heads, head_dim = w_q.shape
        cols = my_heads * head_dim
        qkv_cols = 3 * cols
        my_rows = qkv_cols + cols
        hid = w_1.shape[1]
        images, patches = x.shape[0] // tp, x.shape[1] * tp
        tokens = images * patches

        def to_images(t):
            return lax.all_to_all(t.reshape(tp, images, patches // tp, width), 'tp', 0, 0, tiled=True)

        def join_tokens(blocks):
            return blocks.swapaxes(0, 1).reshape(tokens, width)

        def to_tokens(t):
            return lax.all_to_all(t.reshape(images, patches, width), 'tp', 1, 0, tiled=True)

        def token_sum(t):
            return jnp.sum(t, axis=0, dtype=F32)

        def both(mine, token=None):
            return mine, swap(mine if token is None else after((mine,), token)[0])

        def place(parts, rows):
            low, placed = jnp.array(-jnp.inf, BF16), None
            for t, start in parts:
                spans = [(start, rows - start - t.shape[0], 0)] + [(0, 0, 0)] * (t.ndim - 1)
                padded = lax.pad(t, low, spans)
                placed = padded if placed is None else jnp.maximum(placed, padded)
            return placed

        rest = width - qkv_cols - hid
        bias_row = place([(b_q.reshape(cols), 0), (jnp.zeros((cols,), BF16), cols), (b_v.reshape(cols), 2 * cols), (b_1, qkv_cols),
                          (jnp.zeros((rest,), BF16), width - rest)], width)
        pieces = [w_q.reshape(width, cols).T, w_k.reshape(width, cols).T, w_v.reshape(width, cols).T, w_o.reshape(cols, width)]
        qkv_rows = place([(t, i * cols) for i, t in enumerate(pieces)]
                         + [(jnp.broadcast_to(bias_row[None], (PAD, width)), my_rows)], my_rows + PAD)
        packed = both(gather_rows(qkv_rows))
        x_img = lax.optimization_barrier(join_tokens(to_images(x)))
        w1_mine, w2_mine = gather_rows(w_1.T), gather_rows(w_2)

        w_qkv, wo, b_qkv, b_1_all = [], [], [], []
        for half in packed:
            blocks = half.reshape(chips, my_rows + PAD, width)
            w_qkv.append(blocks[:, :qkv_cols].reshape(chips * qkv_cols, width))
            wo.append(blocks[:, qkv_cols:my_rows].reshape(chips * cols, width))
            b_qkv.append(blocks[:, my_rows, :qkv_cols].reshape(chips * qkv_cols).astype(F32))
            b_1_all.append(blocks[:, my_rows, qkv_cols:qkv_cols + hid].reshape(chips * hid).astype(F32))

        x_f32 = x_img.astype(F32)
        h_one_f, ln1_pull = jax.vjp(layer_norm, x_f32, ln1_gain, ln1_bias)
        h_one = h_one_f.astype(BF16)
        qkv = [(dot(h_one, w, 1, 1) + b).astype(BF16) for w, b in zip(w_qkv, b_qkv)]
        d_moved = to_images(after((d_out,), qkv[0])[0])
        mixed = [attend(t, images, my_heads, head_dim) for t in qkv]
        x_mid = (x_f32 + dot(mixed[0], wo[0], 1, 0) + dot(mixed[1], wo[1], 1, 0) + b_o.astype(F32)).astype(BF16)
        w1 = both(w1_mine, x_mid)
        mid_f32 = x_mid.astype(F32)
        h_two_f, ln2_pull = jax.vjp(layer_norm, mid_f32, ln2_gain, ln2_bias)
        h_two = h_two_f.astype(BF16)
        pre_act = [(dot(h_two, w, 1, 1) + b).astype(BF16) for w, b in zip(w1, b_1_all)]
        gelus = [jax.vjp(gelu_tanh, t.astype(F32)) for t in pre_act]
        hidden = [g[0].astype(BF16) for g in gelus]

        d_out_img = lax.optimization_barrier(join_tokens(after((d_moved,), hidden[0])[0]))
        theirs_2 = dot(hidden[1], d_out_img, 0, 0)
        sum_2 = dot(hidden[0], d_out_img, 0, 0) + swap(theirs_2)
        grad_w_2 = scatter_rows(sum_2).astype(BF16)
        w2 = both(w2_mine, sum_2)
        d_first = dot(d_out_img, after(w2[:1], sum_2)[0], 1, 1).astype(BF16)
        d_hidden = [d_first, dot(d_out_img, after(w2[1:], d_first)[0], 1, 1).astype(BF16)]
        d_pre = [g[1](d.astype(F32))[0].astype(BF16) for g, d in zip(gelus, d_hidden)]
        d_pre_sums = [token_sum(t) for t in d_pre]
        (h_two_late,) = after((h_two,), sum_2)
        theirs_1 = dot(d_pre[1], h_two_late, 0, 0)
        w1_late = after(w1, theirs_1)
        d_h_two = (dot(d_pre[0], w1_late[0], 1, 0) + dot(d_pre[1], w1_late[1], 1, 0)).astype(BF16)
        sum_1 = dot(d_pre[0], h_two_late, 0, 0) + swap(theirs_1)
        grad_w_1 = scatter_rows(sum_1).astype(BF16).T
        w2_late = after(w2, sum_1)
        y_img = (mid_f32 + dot(hidden[0], w2_late[0], 1, 0) + dot(hidden[1], w2_late[1], 1, 0) + b_2.astype(F32)).astype(BF16)
        y_out = to_tokens(y_img)
        d_mid_ln, g_ln2_gain, g_ln2_bias = ln2_pull(d_h_two.astype(F32))
        d_mid = (d_out_img.astype(F32) + d_mid_ln).astype(BF16)
        mixed_late = after(mixed, sum_1)
        theirs_o = dot(mixed_late[1], d_mid, 0, 0)
        d_mixed = [dot(d_mid, w, 1, 1).astype(BF16) for w in wo]
        sum_o = dot(mixed_late[0], d_mid, 0, 0) + swap(theirs_o)
        qkv_late = after(qkv, sum_o)
        d_qkv = [attend_back(t, d, images, my_heads, head_dim) for t, d in zip(qkv_late, d_mixed)]
        theirs_qkv = dot(d_qkv[1], h_one, 0, 0)
        w_qkv_late = after(w_qkv, theirs_qkv)
        d_h_one = (dot(d_qkv[0], w_qkv_late[0], 1, 0) + dot(d_qkv[1], w_qkv_late[1], 1, 0)).astype(BF16)
        sum_qkv = dot(d_qkv[0], h_one, 0, 0) + swap(theirs_qkv)
        sum_all = jnp.concatenate([sum_qkv.reshape(chips, qkv_cols, width), sum_o.reshape(chips, cols, width)], axis=1)
        g_all = scatter_rows(sum_all.reshape(chips * my_rows, width))
        grad_w_o = g_all[qkv_cols:].astype(BF16).reshape(my_heads, head_dim, width)
        g_qkv = g_all[:qkv_cols].reshape(3, cols, width)
        grad_w_q, grad_w_k, grad_w_v = (g_qkv[i].T.astype(BF16).reshape(width, my_heads, head_dim) for i in range(3))
        d_in_ln, g_ln1_gain, g_ln1_bias = ln1_pull(d_h_one.astype(F32))
        grad_x = to_tokens((d_mid.astype(F32) + d_in_ln).astype(BF16))

        me = lax.axis_index('tp')
        core, chip = lax.rem(me, 2), me // 2

        def halves(sums):
            first = jnp.where(core == 0, sums[0], sums[1])
            second = jnp.where(core == 0, sums[1], sums[0])
            return [first, second]

        vecs = jnp.concatenate([g_ln1_gain, g_ln1_bias, token_sum(d_mid), g_ln2_gain, g_ln2_bias, token_sum(d_out_img)]
                               + halves([token_sum(t) for t in d_qkv]) + halves(d_pre_sums))
        sums = sum_over_tp(vecs.reshape(-1, width), tp).reshape(-1)
        six = [sums[i * width:(i + 1) * width] for i in range(6)]
        base = 6 * width
        g_b_qkv = lax.dynamic_slice(sums, (base + (core * chips + chip) * qkv_cols,), (qkv_cols,)).astype(BF16)
        grad_b_q = g_b_qkv[:cols].reshape(my_heads, head_dim)
        grad_b_v = g_b_qkv[2 * cols:].reshape(my_heads, head_dim)
        base += tp * qkv_cols
        grad_b_1 = lax.dynamic_slice(sums, (base + (core * chips + chip) * hid,), (hid,)).astype(BF16)
        return (y_out, grad_x, six[0], six[1], grad_w_q, grad_b_q, grad_w_k, grad_w_v, grad_b_v, grad_w_o,
                six[2].astype(BF16), six[3], six[4], grad_w_1, grad_b_1, grad_w_2, six[5].astype(BF16))

    return jax.shard_map(layer_body, mesh=mesh, in_specs=in_specs, out_specs=out_specs, check_vma=False)
```

```python
import functools
import math
import jax
import jax.numpy as jnp
from jax import lax
from jax.experimental import pallas as pl
from jax.experimental.pallas import tpu as pltpu
from jax.sharding import PartitionSpec as P

LN_EPS = 1e-6
F32 = jnp.float32
BF16 = jnp.bfloat16
PAD = 16


def layer_norm(rows, ln_gain, ln_bias):
    row_mean = jnp.mean(rows, axis=-1, keepdims=True)
    centered = rows - row_mean
    variance = jnp.mean(centered * centered, axis=-1, keepdims=True)
    return centered * lax.rsqrt(variance + LN_EPS) * ln_gain + ln_bias


def gelu_tanh(pre_act):
    return jax.nn.gelu(pre_act, approximate=True)


def after(values, token):
    return lax.optimization_barrier((*values, token))[:len(values)]


def dot(a, b, ca, cb):
    return lax.dot_general(a, b, (((ca,), (cb,)), ((), ())), preferred_element_type=F32)


def head_lanes(shape, head, head_dim):
    lane = lax.broadcasted_iota(jnp.int32, shape, 1)
    return (lane >= head * head_dim) & (lane < (head + 1) * head_dim)


def attend_kernel(blocks, heads, head_dim, qkv_ref, out_ref):
    cols = heads * head_dim
    scale = 1.0 / math.sqrt(head_dim)
    for block in range(blocks):
        base = block * 3 * cols
        q, k, v = (qkv_ref[:, base + i * cols:base + (i + 1) * cols] for i in range(3))
        total = None
        for head in range(heads):
            mine = head_lanes(q.shape, head, head_dim)
            s = dot(jnp.where(mine, q, jnp.zeros_like(q)), k, 1, 1) * scale
            e = jnp.exp(s - jnp.max(s, axis=1, keepdims=True))
            p = (e * (1.0 / jnp.sum(e, axis=1, keepdims=True))).astype(BF16)
            a = dot(p, v, 1, 0)
            total = a if total is None else jnp.where(mine, a, total)
        out_ref[:, block * cols:(block + 1) * cols] = total.astype(BF16)


def attend_back_kernel(blocks, heads, head_dim, qkv_ref, da_ref, dqkv_ref):
    cols = heads * head_dim
    scale = 1.0 / math.sqrt(head_dim)
    for block in range(blocks):
        base = block * 3 * cols
        q, k, v = (qkv_ref[:, base + i * cols:base + (i + 1) * cols] for i in range(3))
        da = da_ref[:, block * cols:(block + 1) * cols]
        dq = dk = dv = None
        for head in range(heads):
            mine = head_lanes(q.shape, head, head_dim)
            zero = jnp.zeros_like(q)
            s = dot(jnp.where(mine, k, zero), q, 1, 1) * scale
            e = jnp.exp(s - jnp.max(s, axis=0, keepdims=True))
            p32 = e * (1.0 / jnp.sum(e, axis=0, keepdims=True))
            dv_h = dot(p32.astype(BF16), da, 1, 0)
            dp = dot(jnp.where(mine, v, zero), da, 1, 1).astype(BF16).astype(F32)
            ds = p32 * (dp - jnp.sum(dp * p32, axis=0, keepdims=True))
            ds = (ds * scale).astype(BF16)
            dk_h = dot(ds, q, 1, 0)
            dq_h = dot(ds, k, 0, 0)
            if head == 0:
                dq, dk, dv = dq_h, dk_h, dv_h
            else:
                dq, dk, dv = jnp.where(mine, dq_h, dq), jnp.where(mine, dk_h, dk), jnp.where(mine, dv_h, dv)
        for i, d in enumerate((dq, dk, dv)):
            dqkv_ref[:, base + i * cols:base + (i + 1) * cols] = d.astype(BF16)


GROUP = 4


def attend(qkv, images, heads, head_dim):
    tokens, wide = qkv.shape
    patches, cols = tokens // images, heads * head_dim
    blocks = wide // (3 * cols)
    group = min(GROUP, blocks)
    return pl.pallas_call(
        functools.partial(attend_kernel, group, heads, head_dim),
        grid=(images, blocks // group),
        in_specs=[pl.BlockSpec((patches, group * 3 * cols), lambda i, j: (i, j))],
        out_specs=pl.BlockSpec((patches, group * cols), lambda i, j: (i, j)),
        out_shape=jax.ShapeDtypeStruct((tokens, blocks * cols), BF16),
        cost_estimate=pl.CostEstimate(flops=images * blocks * heads * patches * patches * 1024, bytes_accessed=8 * tokens * blocks * cols,
                                      transcendentals=0),
        name="attend",
    )(qkv)


def attend_back(qkv, d_mixed, images, heads, head_dim):
    tokens, wide = qkv.shape
    patches, cols = tokens // images, heads * head_dim
    blocks = wide // (3 * cols)
    group = min(GROUP, blocks)
    return pl.pallas_call(
        functools.partial(attend_back_kernel, group, heads, head_dim),
        grid=(images, blocks // group),
        in_specs=[pl.BlockSpec((patches, group * 3 * cols), lambda i, j: (i, j)),
                  pl.BlockSpec((patches, group * cols), lambda i, j: (i, j))],
        out_specs=pl.BlockSpec((patches, group * 3 * cols), lambda i, j: (i, j)),
        out_shape=jax.ShapeDtypeStruct((tokens, wide), BF16),
        cost_estimate=pl.CostEstimate(flops=images * blocks * heads * patches * patches * 2048, bytes_accessed=14 * tokens * blocks * cols,
                                      transcendentals=0),
        name="attend_back",
    )(qkv, d_mixed)


def sum_kernel(n, vec_ref, out_ref, slots, send_sems, recv_sems, local_sem):
    me = lax.axis_index('tp')
    barrier = pltpu.get_barrier_semaphore()
    for step in range(1, n):
        pl.semaphore_signal(barrier, inc=1, device_id={'tp': lax.rem(me + step, n)}, device_id_type=pl.DeviceIdType.MESH)
    pl.semaphore_wait(barrier, n - 1)
    own = pltpu.make_async_copy(vec_ref, slots.at[me], local_sem)
    own.start()
    copies = [pltpu.make_async_remote_copy(src_ref=vec_ref, dst_ref=slots.at[me], send_sem=send_sems.at[step - 1],
                                           recv_sem=recv_sems.at[step - 1], device_id={'tp': lax.rem(me + step, n)},
                                           device_id_type=pl.DeviceIdType.MESH) for step in range(1, n)]
    for copy in copies:
        copy.start()
    own.wait()
    for copy in copies:
        copy.wait()
    total = slots[0]
    for i in range(1, n):
        total = total + slots[i]
    out_ref[...] = total


def sum_over_tp(vecs, n):
    return pl.pallas_call(
        functools.partial(sum_kernel, n),
        out_shape=jax.ShapeDtypeStruct(vecs.shape, F32),
        in_specs=[pl.BlockSpec(memory_space=pltpu.VMEM)],
        out_specs=pl.BlockSpec(memory_space=pltpu.VMEM),
        scratch_shapes=[pltpu.VMEM((n, *vecs.shape), F32), pltpu.SemaphoreType.DMA((n - 1,)), pltpu.SemaphoreType.DMA((n - 1,)),
                        pltpu.SemaphoreType.DMA],
        compiler_params=pltpu.CompilerParams(collective_id=0, has_side_effects=True),
        name="sum_over_tp",
    )(vecs)


def solution(mesh):
    act_spec = P('dp', 'tp', None)
    replicated = P()
    head_w = P(None, 'tp', None)
    head_b = P('tp', None)
    grad_head_w = P('dp', 'tp', None)
    grad_head_b = P(('dp', 'tp'), None)
    grad_vec = P('dp')
    in_specs = (act_spec, act_spec, replicated, replicated, head_w, head_b, head_w, head_w, head_b,
                P('tp', None, None), replicated, replicated, replicated, P(None, 'tp'), P('tp'), P('tp', None), replicated)
    out_specs = (act_spec, act_spec, grad_vec, grad_vec, grad_head_w, grad_head_b, grad_head_w, grad_head_w, grad_head_b,
                 P(('dp', 'tp'), None, None), grad_vec, grad_vec, grad_vec, P('dp', 'tp'), P(('dp', 'tp')),
                 P(('dp', 'tp'), None), grad_vec)
    tp = mesh.shape['tp']
    chips = tp // 2
    rings = [[2 * i + core for i in range(chips)] for core in range(2)]
    pairs = [(i, i + 1 - 2 * (i % 2)) for i in range(tp)]

    def gather_rows(rows):
        return lax.all_gather(rows, 'tp', axis=0, tiled=True, axis_index_groups=rings)

    def scatter_rows(rows):
        return lax.psum_scatter(rows, 'tp', scatter_dimension=0, tiled=True, axis_index_groups=rings)

    def shift(t, chip_steps):
        return lax.ppermute(t, 'tp', [(i, (i + 2 * chip_steps) % tp) for i in range(tp)])

    def swap(t):
        return lax.ppermute(t, 'tp', pairs)

    def layer_body(x, d_out, ln1_gain, ln1_bias, w_q, b_q, w_k, w_v, b_v, w_o, b_o, ln2_gain, ln2_bias, w_1, b_1, w_2, b_2):
        width, my_heads, head_dim = w_q.shape
        cols = my_heads * head_dim
        qkv_cols = 3 * cols
        my_rows = qkv_cols + cols
        hid = w_1.shape[1]
        images, patches = x.shape[0] // tp, x.shape[1] * tp
        tokens = images * patches

        def to_images(t):
            return lax.all_to_all(t.reshape(tp, images, patches // tp, width), 'tp', 0, 0, tiled=True)

        def join_tokens(blocks):
            return blocks.swapaxes(0, 1).reshape(tokens, width)

        def to_tokens(t):
            return lax.all_to_all(t.reshape(images, patches, width), 'tp', 1, 0, tiled=True)

        def token_sum(t):
            return jnp.sum(t, axis=0, dtype=F32)

        def both(mine, token=None):
            return mine, swap(mine if token is None else after((mine,), token)[0])

        def place(parts, rows):
            low, placed = jnp.array(-jnp.inf, BF16), None
            for t, start in parts:
                spans = [(start, rows - start - t.shape[0], 0)] + [(0, 0, 0)] * (t.ndim - 1)
                padded = lax.pad(t, low, spans)
                placed = padded if placed is None else jnp.maximum(placed, padded)
            return placed

        rest = width - qkv_cols - hid
        bias_row = place([(b_q.reshape(cols), 0), (jnp.zeros((cols,), BF16), cols), (b_v.reshape(cols), 2 * cols), (b_1, qkv_cols),
                          (jnp.zeros((rest,), BF16), width - rest)], width)
        pieces = [w_q.reshape(width, cols).T, w_k.reshape(width, cols).T, w_v.reshape(width, cols).T, w_o.reshape(cols, width)]
        qkv_rows = place([(t, i * cols) for i, t in enumerate(pieces)]
                         + [(jnp.broadcast_to(bias_row[None], (PAD, width)), my_rows)], my_rows + PAD)
        packed = both(gather_rows(qkv_rows))
        me = lax.axis_index('tp')
        core, chip = lax.rem(me, 2), me // 2
        x_img = lax.optimization_barrier(join_tokens(to_images(x)))
        w1_mine = gather_rows(w_1.T)

        w_qkv, wo, b_qkv, b_1_all = [], [], [], []
        for half in packed:
            blocks = half.reshape(chips, my_rows + PAD, width)
            w_qkv.append(blocks[:, :qkv_cols].reshape(chips * qkv_cols, width))
            wo.append(blocks[:, qkv_cols:my_rows].reshape(chips * cols, width))
            b_qkv.append(blocks[:, my_rows, :qkv_cols].reshape(chips * qkv_cols).astype(F32))
            b_1_all.append(blocks[:, my_rows, qkv_cols:qkv_cols + hid].reshape(chips * hid).astype(F32))

        x_f32 = x_img.astype(F32)
        h_one_f, ln1_pull = jax.vjp(layer_norm, x_f32, ln1_gain, ln1_bias)
        h_one = h_one_f.astype(BF16)
        qkv_mine = (dot(h_one, w_qkv[0], 1, 1) + b_qkv[0]).astype(BF16)
        mixed_mine = attend(qkv_mine, images, my_heads, head_dim)
        d_moved = to_images(after((d_out,), mixed_mine)[0])
        qkv_theirs = (dot(h_one, w_qkv[1], 1, 1) + b_qkv[1]).astype(BF16)
        mixed_theirs = attend(qkv_theirs, images, my_heads, head_dim)
        qkv, mixed = [qkv_mine, qkv_theirs], [mixed_mine, mixed_theirs]
        (w_2_late,) = after((w_2,), mixed_theirs)
        steps = sorted(range(1, chips), key=lambda k: min(k, chips - k))
        w2_pieces = [shift(w_2_late, k) for k in steps]
        x_mid = (x_f32 + dot(mixed[0], wo[0], 1, 0) + dot(mixed[1], wo[1], 1, 0) + b_o.astype(F32)).astype(BF16)
        w1 = both(w1_mine, x_mid)
        mid_f32 = x_mid.astype(F32)
        h_two_f, ln2_pull = jax.vjp(layer_norm, mid_f32, ln2_gain, ln2_bias)
        h_two = h_two_f.astype(BF16)

        def mlp_up(rows, half):
            pre_act = (dot(rows, w1[half], 1, 1) + b_1_all[half]).astype(BF16)
            return jax.vjp(gelu_tanh, pre_act.astype(F32))

        gelu_theirs = mlp_up(h_two, 1)
        hidden_theirs = gelu_theirs[0].astype(BF16)
        d_out_img = lax.optimization_barrier(join_tokens(after((d_moved,), hidden_theirs)[0]))
        theirs_2 = dot(hidden_theirs, d_out_img, 0, 0)
        gelus = [mlp_up(after((h_two,), theirs_2)[0], 0), gelu_theirs]
        hidden = [gelus[0][0].astype(BF16), hidden_theirs]
        sum_2 = dot(hidden[0], d_out_img, 0, 0) + swap(theirs_2)
        grad_w_2 = scatter_rows(sum_2).astype(BF16)
        (d_out_late,) = after((d_out_img,), sum_2)
        d_out_sum = lax.optimization_barrier(token_sum(d_out_late))
        w2_mine = jnp.zeros((chips * hid, width), BF16)
        for k, piece in zip([0, *steps], after((w_2_late, *w2_pieces), sum_2)):
            w2_mine = lax.dynamic_update_slice(w2_mine, piece, (lax.rem(chip + chips - k, chips) * hid, 0))
        w2 = both(w2_mine)
        d_first = dot(d_out_img, after(w2[:1], sum_2)[0], 1, 1).astype(BF16)
        d_hidden = [d_first, dot(d_out_img, after(w2[1:], d_first)[0], 1, 1).astype(BF16)]
        d_pre = [g[1](d.astype(F32))[0].astype(BF16) for g, d in zip(gelus, d_hidden)]
        d_pre_sums = [token_sum(t) for t in d_pre]
        (h_two_late,) = after((h_two,), sum_2)
        theirs_1 = dot(d_pre[1], h_two_late, 0, 0)
        w1_late = after(w1, theirs_1)
        d_h_two = (dot(d_pre[0], w1_late[0], 1, 0) + dot(d_pre[1], w1_late[1], 1, 0)).astype(BF16)
        sum_1 = dot(d_pre[0], h_two_late, 0, 0) + swap(theirs_1)
        grad_w_1 = scatter_rows(sum_1).astype(BF16).T
        w2_late = after(w2, sum_1)
        y_img = (mid_f32 + dot(hidden[0], w2_late[0], 1, 0) + dot(hidden[1], w2_late[1], 1, 0) + b_2.astype(F32)).astype(BF16)
        y_out = to_tokens(y_img)
        (d_h_two,) = after((d_h_two,), y_img)
        d_mid_ln, g_ln2_gain, g_ln2_bias = ln2_pull(d_h_two.astype(F32))
        d_mid = (d_out_img.astype(F32) + d_mid_ln).astype(BF16)
        mixed_late = after(mixed, sum_1)
        theirs_o = dot(mixed_late[1], d_mid, 0, 0)
        d_mixed = [dot(d_mid, w, 1, 1).astype(BF16) for w in wo]
        sum_o = dot(mixed_late[0], d_mid, 0, 0) + swap(theirs_o)
        qkv_late = after(qkv, sum_o)
        d_qkv = [attend_back(t, d, images, my_heads, head_dim) for t, d in zip(qkv_late, d_mixed)]
        theirs_qkv = dot(d_qkv[1], h_one, 0, 0)
        w_qkv_late = after(w_qkv, theirs_qkv)
        d_h_one = (dot(d_qkv[0], w_qkv_late[0], 1, 0) + dot(d_qkv[1], w_qkv_late[1], 1, 0)).astype(BF16)
        sum_qkv = dot(d_qkv[0], h_one, 0, 0) + swap(theirs_qkv)
        d_in_ln, g_ln1_gain, g_ln1_bias = ln1_pull(d_h_one.astype(F32))
        grad_x_img = (d_mid.astype(F32) + d_in_ln).astype(BF16)
        grad_x = to_tokens(grad_x_img)
        sum_all = jnp.concatenate([sum_qkv.reshape(chips, qkv_cols, width), sum_o.reshape(chips, cols, width)], axis=1)
        g_all = scatter_rows(sum_all.reshape(chips * my_rows, width))
        grad_w_o = g_all[qkv_cols:].astype(BF16).reshape(my_heads, head_dim, width)
        g_qkv = g_all[:qkv_cols].reshape(3, cols, width)
        grad_w_q, grad_w_k, grad_w_v = (g_qkv[i].T.astype(BF16).reshape(width, my_heads, head_dim) for i in range(3))

        def halves(sums):
            first = jnp.where(core == 0, sums[0], sums[1])
            second = jnp.where(core == 0, sums[1], sums[0])
            return [first, second]

        vecs = jnp.concatenate([g_ln1_gain, g_ln1_bias, token_sum(d_mid), g_ln2_gain, g_ln2_bias, d_out_sum]
                               + halves([token_sum(t) for t in d_qkv]) + halves(d_pre_sums))
        sums = sum_over_tp(vecs.reshape(-1, width), tp).reshape(-1)
        six = [sums[i * width:(i + 1) * width] for i in range(6)]
        base = 6 * width
        g_b_qkv = lax.dynamic_slice(sums, (base + (core * chips + chip) * qkv_cols,), (qkv_cols,)).astype(BF16)
        grad_b_q = g_b_qkv[:cols].reshape(my_heads, head_dim)
        grad_b_v = g_b_qkv[2 * cols:].reshape(my_heads, head_dim)
        base += tp * qkv_cols
        grad_b_1 = lax.dynamic_slice(sums, (base + (core * chips + chip) * hid,), (hid,)).astype(BF16)
        return (y_out, grad_x, six[0], six[1], grad_w_q, grad_b_q, grad_w_k, grad_w_v, grad_b_v, grad_w_o,
                six[2].astype(BF16), six[3], six[4], grad_w_1, grad_b_1, grad_w_2, six[5].astype(BF16))

    return jax.shard_map(layer_body, mesh=mesh, in_specs=in_specs, out_specs=out_specs, check_vma=False)
```

```python
import functools
import math
import jax
import jax.numpy as jnp
from jax import lax
from jax.experimental import pallas as pl
from jax.experimental.pallas import tpu as pltpu
from jax.sharding import PartitionSpec as P

LN_EPS = 1e-6
F32 = jnp.float32
BF16 = jnp.bfloat16
PAD = 16


def layer_norm(rows, ln_gain, ln_bias):
    row_mean = jnp.mean(rows, axis=-1, keepdims=True)
    centered = rows - row_mean
    variance = jnp.mean(centered * centered, axis=-1, keepdims=True)
    return centered * lax.rsqrt(variance + LN_EPS) * ln_gain + ln_bias


def gelu_tanh(pre_act):
    return jax.nn.gelu(pre_act, approximate=True)


def after(values, token):
    return lax.optimization_barrier((*values, token))[:len(values)]


def dot(a, b, ca, cb):
    return lax.dot_general(a, b, (((ca,), (cb,)), ((), ())), preferred_element_type=F32)


def head_lanes(shape, head, head_dim):
    lane = lax.broadcasted_iota(jnp.int32, shape, 1)
    return (lane >= head * head_dim) & (lane < (head + 1) * head_dim)


def attend_kernel(blocks, heads, head_dim, qkv_ref, out_ref):
    cols = heads * head_dim
    scale = 1.0 / math.sqrt(head_dim)
    for block in range(blocks):
        base = block * 3 * cols
        q, k, v = (qkv_ref[:, base + i * cols:base + (i + 1) * cols] for i in range(3))
        total = None
        for head in range(heads):
            mine = head_lanes(q.shape, head, head_dim)
            s = dot(jnp.where(mine, q, jnp.zeros_like(q)), k, 1, 1) * scale
            e = jnp.exp(s - jnp.max(s, axis=1, keepdims=True))
            p = (e * (1.0 / jnp.sum(e, axis=1, keepdims=True))).astype(BF16)
            a = dot(p, v, 1, 0)
            total = a if total is None else jnp.where(mine, a, total)
        out_ref[:, block * cols:(block + 1) * cols] = total.astype(BF16)


def attend_back_kernel(blocks, heads, head_dim, qkv_ref, da_ref, dqkv_ref):
    cols = heads * head_dim
    scale = 1.0 / math.sqrt(head_dim)
    for block in range(blocks):
        base = block * 3 * cols
        q, k, v = (qkv_ref[:, base + i * cols:base + (i + 1) * cols] for i in range(3))
        da = da_ref[:, block * cols:(block + 1) * cols]
        dq = dk = dv = None
        for head in range(heads):
            mine = head_lanes(q.shape, head, head_dim)
            zero = jnp.zeros_like(q)
            s = dot(jnp.where(mine, k, zero), q, 1, 1) * scale
            e = jnp.exp(s - jnp.max(s, axis=0, keepdims=True))
            p32 = e * (1.0 / jnp.sum(e, axis=0, keepdims=True))
            dv_h = dot(p32.astype(BF16), da, 1, 0)
            dp = dot(jnp.where(mine, v, zero), da, 1, 1).astype(BF16).astype(F32)
            ds = p32 * (dp - jnp.sum(dp * p32, axis=0, keepdims=True))
            ds = (ds * scale).astype(BF16)
            dk_h = dot(ds, q, 1, 0)
            dq_h = dot(ds, k, 0, 0)
            if head == 0:
                dq, dk, dv = dq_h, dk_h, dv_h
            else:
                dq, dk, dv = jnp.where(mine, dq_h, dq), jnp.where(mine, dk_h, dk), jnp.where(mine, dv_h, dv)
        for i, d in enumerate((dq, dk, dv)):
            dqkv_ref[:, base + i * cols:base + (i + 1) * cols] = d.astype(BF16)


GROUP = 4


def attend(qkv, images, heads, head_dim):
    tokens, wide = qkv.shape
    patches, cols = tokens // images, heads * head_dim
    blocks = wide // (3 * cols)
    group = min(GROUP, blocks)
    return pl.pallas_call(
        functools.partial(attend_kernel, group, heads, head_dim),
        grid=(images, blocks // group),
        in_specs=[pl.BlockSpec((patches, group * 3 * cols), lambda i, j: (i, j))],
        out_specs=pl.BlockSpec((patches, group * cols), lambda i, j: (i, j)),
        out_shape=jax.ShapeDtypeStruct((tokens, blocks * cols), BF16),
        cost_estimate=pl.CostEstimate(flops=images * blocks * heads * patches * patches * 1024, bytes_accessed=8 * tokens * blocks * cols,
                                      transcendentals=0),
        name="attend",
    )(qkv)


def attend_back(qkv, d_mixed, images, heads, head_dim):
    tokens, wide = qkv.shape
    patches, cols = tokens // images, heads * head_dim
    blocks = wide // (3 * cols)
    group = min(GROUP, blocks)
    return pl.pallas_call(
        functools.partial(attend_back_kernel, group, heads, head_dim),
        grid=(images, blocks // group),
        in_specs=[pl.BlockSpec((patches, group * 3 * cols), lambda i, j: (i, j)),
                  pl.BlockSpec((patches, group * cols), lambda i, j: (i, j))],
        out_specs=pl.BlockSpec((patches, group * 3 * cols), lambda i, j: (i, j)),
        out_shape=jax.ShapeDtypeStruct((tokens, wide), BF16),
        cost_estimate=pl.CostEstimate(flops=images * blocks * heads * patches * patches * 2048, bytes_accessed=14 * tokens * blocks * cols,
                                      transcendentals=0),
        name="attend_back",
    )(qkv, d_mixed)


def sum_kernel(n, vec_ref, out_ref, slots, send_sems, recv_sems, local_sem):
    me = lax.axis_index('tp')
    barrier = pltpu.get_barrier_semaphore()
    for step in range(1, n):
        pl.semaphore_signal(barrier, inc=1, device_id={'tp': lax.rem(me + step, n)}, device_id_type=pl.DeviceIdType.MESH)
    pl.semaphore_wait(barrier, n - 1)
    own = pltpu.make_async_copy(vec_ref, slots.at[me], local_sem)
    own.start()
    copies = [pltpu.make_async_remote_copy(src_ref=vec_ref, dst_ref=slots.at[me], send_sem=send_sems.at[step - 1],
                                           recv_sem=recv_sems.at[step - 1], device_id={'tp': lax.rem(me + step, n)},
                                           device_id_type=pl.DeviceIdType.MESH) for step in range(1, n)]
    for copy in copies:
        copy.start()
    own.wait()
    for copy in copies:
        copy.wait()
    total = slots[0]
    for i in range(1, n):
        total = total + slots[i]
    out_ref[...] = total


def sum_over_tp(vecs, n):
    return pl.pallas_call(
        functools.partial(sum_kernel, n),
        out_shape=jax.ShapeDtypeStruct(vecs.shape, F32),
        in_specs=[pl.BlockSpec(memory_space=pltpu.VMEM)],
        out_specs=pl.BlockSpec(memory_space=pltpu.VMEM),
        scratch_shapes=[pltpu.VMEM((n, *vecs.shape), F32), pltpu.SemaphoreType.DMA((n - 1,)), pltpu.SemaphoreType.DMA((n - 1,)),
                        pltpu.SemaphoreType.DMA],
        compiler_params=pltpu.CompilerParams(collective_id=0, has_side_effects=True),
        name="sum_over_tp",
    )(vecs)


def solution(mesh):
    act_spec = P('dp', 'tp', None)
    replicated = P()
    head_w = P(None, 'tp', None)
    head_b = P('tp', None)
    grad_head_w = P('dp', 'tp', None)
    grad_head_b = P(('dp', 'tp'), None)
    grad_vec = P('dp')
    in_specs = (act_spec, act_spec, replicated, replicated, head_w, head_b, head_w, head_w, head_b,
                P('tp', None, None), replicated, replicated, replicated, P(None, 'tp'), P('tp'), P('tp', None), replicated)
    out_specs = (act_spec, act_spec, grad_vec, grad_vec, grad_head_w, grad_head_b, grad_head_w, grad_head_w, grad_head_b,
                 P(('dp', 'tp'), None, None), grad_vec, grad_vec, grad_vec, P('dp', 'tp'), P(('dp', 'tp')),
                 P(('dp', 'tp'), None), grad_vec)
    tp = mesh.shape['tp']
    chips = tp // 2
    rings = [[2 * i + core for i in range(chips)] for core in range(2)]
    pairs = [(i, i + 1 - 2 * (i % 2)) for i in range(tp)]

    def gather_rows(rows):
        return lax.all_gather(rows, 'tp', axis=0, tiled=True, axis_index_groups=rings)

    def scatter_rows(rows):
        return lax.psum_scatter(rows, 'tp', scatter_dimension=0, tiled=True, axis_index_groups=rings)

    def swap(t):
        return lax.ppermute(t, 'tp', pairs)

    def layer_body(x, d_out, ln1_gain, ln1_bias, w_q, b_q, w_k, w_v, b_v, w_o, b_o, ln2_gain, ln2_bias, w_1, b_1, w_2, b_2):
        width, my_heads, head_dim = w_q.shape
        cols = my_heads * head_dim
        qkv_cols = 3 * cols
        my_rows = qkv_cols + cols
        hid = w_1.shape[1]
        images, patches = x.shape[0] // tp, x.shape[1] * tp
        tokens = images * patches

        def to_images(t):
            return lax.all_to_all(t.reshape(tp, images, patches // tp, width), 'tp', 0, 0, tiled=True)

        def join_tokens(blocks):
            return blocks.swapaxes(0, 1).reshape(tokens, width)

        def to_tokens(t):
            return lax.all_to_all(t.reshape(images, patches, width), 'tp', 1, 0, tiled=True)

        def token_sum(t):
            return jnp.sum(t, axis=0, dtype=F32)

        def both(mine, token=None):
            return mine, swap(mine if token is None else after((mine,), token)[0])

        def place(parts, rows):
            low, placed = jnp.array(-jnp.inf, BF16), None
            for t, start in parts:
                spans = [(start, rows - start - t.shape[0], 0)] + [(0, 0, 0)] * (t.ndim - 1)
                padded = lax.pad(t, low, spans)
                placed = padded if placed is None else jnp.maximum(placed, padded)
            return placed

        rest = width - qkv_cols - hid
        bias_row = place([(b_q.reshape(cols), 0), (jnp.zeros((cols,), BF16), cols), (b_v.reshape(cols), 2 * cols), (b_1, qkv_cols),
                          (jnp.zeros((rest,), BF16), width - rest)], width)
        pieces = [w_q.reshape(width, cols).T, w_k.reshape(width, cols).T, w_v.reshape(width, cols).T, w_o.reshape(cols, width)]
        qkv_rows = place([(t, i * cols) for i, t in enumerate(pieces)]
                         + [(jnp.broadcast_to(bias_row[None], (PAD, width)), my_rows)], my_rows + PAD)
        packed = both(gather_rows(qkv_rows))
        x_img = lax.optimization_barrier(join_tokens(to_images(x)))
        w1_mine, w2_mine = gather_rows(w_1.T), gather_rows(w_2)

        w_qkv, wo, b_qkv, b_1_all = [], [], [], []
        for half in packed:
            blocks = half.reshape(chips, my_rows + PAD, width)
            w_qkv.append(blocks[:, :qkv_cols].reshape(chips * qkv_cols, width))
            wo.append(blocks[:, qkv_cols:my_rows].reshape(chips * cols, width))
            b_qkv.append(blocks[:, my_rows, :qkv_cols].reshape(chips * qkv_cols).astype(F32))
            b_1_all.append(blocks[:, my_rows, qkv_cols:qkv_cols + hid].reshape(chips * hid).astype(F32))

        x_f32 = x_img.astype(F32)
        h_one_f, ln1_pull = jax.vjp(layer_norm, x_f32, ln1_gain, ln1_bias)
        h_one = h_one_f.astype(BF16)
        qkv_mine = (dot(h_one, w_qkv[0], 1, 1) + b_qkv[0]).astype(BF16)
        mixed_mine = attend(qkv_mine, images, my_heads, head_dim)
        d_moved = to_images(after((d_out,), mixed_mine)[0])
        qkv_theirs = (dot(h_one, w_qkv[1], 1, 1) + b_qkv[1]).astype(BF16)
        mixed_theirs = attend(qkv_theirs, images, my_heads, head_dim)
        qkv, mixed = [qkv_mine, qkv_theirs], [mixed_mine, mixed_theirs]
        x_mid = (x_f32 + dot(mixed[0], wo[0], 1, 0) + dot(mixed[1], wo[1], 1, 0) + b_o.astype(F32)).astype(BF16)
        w1 = both(w1_mine, x_mid)
        mid_f32 = x_mid.astype(F32)
        h_two_f, ln2_pull = jax.vjp(layer_norm, mid_f32, ln2_gain, ln2_bias)
        h_two = h_two_f.astype(BF16)

        def mlp_up(rows, half):
            pre_act = (dot(rows, w1[half], 1, 1) + b_1_all[half]).astype(BF16)
            return jax.vjp(gelu_tanh, pre_act.astype(F32))

        gelu_theirs = mlp_up(h_two, 1)
        hidden_theirs = gelu_theirs[0].astype(BF16)
        d_out_img = lax.optimization_barrier(join_tokens(after((d_moved,), hidden_theirs)[0]))
        theirs_2 = dot(hidden_theirs, d_out_img, 0, 0)
        gelus = [mlp_up(after((h_two,), theirs_2)[0], 0), gelu_theirs]
        hidden = [gelus[0][0].astype(BF16), hidden_theirs]
        sum_2 = dot(hidden[0], d_out_img, 0, 0) + swap(theirs_2)
        grad_w_2 = scatter_rows(sum_2).astype(BF16)
        w2 = both(w2_mine, sum_2)
        d_first = dot(d_out_img, after(w2[:1], sum_2)[0], 1, 1).astype(BF16)
        d_hidden = [d_first, dot(d_out_img, after(w2[1:], d_first)[0], 1, 1).astype(BF16)]
        d_pre = [g[1](d.astype(F32))[0].astype(BF16) for g, d in zip(gelus, d_hidden)]
        d_pre_sums = [token_sum(t) for t in d_pre]
        (h_two_late,) = after((h_two,), sum_2)
        theirs_1 = dot(d_pre[1], h_two_late, 0, 0)
        w1_late = after(w1, theirs_1)
        d_h_two = (dot(d_pre[0], w1_late[0], 1, 0) + dot(d_pre[1], w1_late[1], 1, 0)).astype(BF16)
        sum_1 = dot(d_pre[0], h_two_late, 0, 0) + swap(theirs_1)
        grad_w_1 = scatter_rows(sum_1).astype(BF16).T
        w2_late = after(w2, sum_1)
        y_img = (mid_f32 + dot(hidden[0], w2_late[0], 1, 0) + dot(hidden[1], w2_late[1], 1, 0) + b_2.astype(F32)).astype(BF16)
        y_out = to_tokens(y_img)
        (d_h_two,) = after((d_h_two,), y_img)
        d_mid_ln, g_ln2_gain, g_ln2_bias = ln2_pull(d_h_two.astype(F32))
        d_mid = (d_out_img.astype(F32) + d_mid_ln).astype(BF16)
        mixed_late = after(mixed, sum_1)
        theirs_o = dot(mixed_late[1], d_mid, 0, 0)
        d_mixed = [dot(d_mid, w, 1, 1).astype(BF16) for w in wo]
        sum_o = dot(mixed_late[0], d_mid, 0, 0) + swap(theirs_o)
        qkv_late = after(qkv, sum_o)
        d_qkv = [attend_back(t, d, images, my_heads, head_dim) for t, d in zip(qkv_late, d_mixed)]
        theirs_qkv = dot(d_qkv[1], h_one, 0, 0)
        w_qkv_late = after(w_qkv, theirs_qkv)
        d_h_one = (dot(d_qkv[0], w_qkv_late[0], 1, 0) + dot(d_qkv[1], w_qkv_late[1], 1, 0)).astype(BF16)
        sum_qkv = dot(d_qkv[0], h_one, 0, 0) + swap(theirs_qkv)
        d_in_ln, g_ln1_gain, g_ln1_bias = ln1_pull(d_h_one.astype(F32))
        grad_x_img = (d_mid.astype(F32) + d_in_ln).astype(BF16)
        grad_x = to_tokens(grad_x_img)
        sum_o, sum_qkv = after((sum_o, sum_qkv), grad_x_img)
        sum_all = jnp.concatenate([sum_qkv.reshape(chips, qkv_cols, width), sum_o.reshape(chips, cols, width)], axis=1)
        g_all = scatter_rows(sum_all.reshape(chips * my_rows, width))
        grad_w_o = g_all[qkv_cols:].astype(BF16).reshape(my_heads, head_dim, width)
        g_qkv = g_all[:qkv_cols].reshape(3, cols, width)
        grad_w_q, grad_w_k, grad_w_v = (g_qkv[i].T.astype(BF16).reshape(width, my_heads, head_dim) for i in range(3))

        me = lax.axis_index('tp')
        core, chip = lax.rem(me, 2), me // 2

        def halves(sums):
            first = jnp.where(core == 0, sums[0], sums[1])
            second = jnp.where(core == 0, sums[1], sums[0])
            return [first, second]

        vecs = jnp.concatenate([g_ln1_gain, g_ln1_bias, token_sum(d_mid), g_ln2_gain, g_ln2_bias, token_sum(d_out_img)]
                               + halves([token_sum(t) for t in d_qkv]) + halves(d_pre_sums))
        sums = sum_over_tp(vecs.reshape(-1, width), tp).reshape(-1)
        six = [sums[i * width:(i + 1) * width] for i in range(6)]
        base = 6 * width
        g_b_qkv = lax.dynamic_slice(sums, (base + (core * chips + chip) * qkv_cols,), (qkv_cols,)).astype(BF16)
        grad_b_q = g_b_qkv[:cols].reshape(my_heads, head_dim)
        grad_b_v = g_b_qkv[2 * cols:].reshape(my_heads, head_dim)
        base += tp * qkv_cols
        grad_b_1 = lax.dynamic_slice(sums, (base + (core * chips + chip) * hid,), (hid,)).astype(BF16)
        return (y_out, grad_x, six[0], six[1], grad_w_q, grad_b_q, grad_w_k, grad_w_v, grad_b_v, grad_w_o,
                six[2].astype(BF16), six[3], six[4], grad_w_1, grad_b_1, grad_w_2, six[5].astype(BF16))

    return jax.shard_map(layer_body, mesh=mesh, in_specs=in_specs, out_specs=out_specs, check_vma=False)
```
